256 devices in a mesh: tm: 16 (over y, x), lat: 16 (over z, core).
Axes of the slice: x: 4, y: 4, z: 8, core: 2. Of those that a mesh axis runs over, the one named last changes fastest.
Arguments:
- states: float32 [32, 69, 64, 256], P('tm', None, 'lat'), may hold values from -6 to 6
- observed: float32 [32, 69, 64, 256], P('tm', None, 'lat'), may hold values from -6 to 6
- conv_in: bfloat16 [3, 3, 256, 345], replicated, may hold values from -0.109375 to 0.109375
- bias_in: float32 [256], replicated, may hold values from -3 to 3
- conv_out: bfloat16 [3, 3, 69, 256], replicated, may hold values from -0.125 to 0.125
- bias_out: float32 [69], replicated, may hold values from -3 to 3
Outputs:
- scores: float32 [32, 69, 64, 256], P('tm', None, 'lat')
- guidance: float32 [32, 69, 64, 256], P('tm', None, 'lat')
The draws below stay inside these ranges and needn't reach their ends.
All inputs are finite; a program needn't handle non-finite values.
Results may differ from the reference program's by a relative error of at most 0.0045.
Values may be sent and summed in bfloat16 or wider, within the bound.
A program may use at most 64 MiB of HBM per device.

```python
import jax
import jax.numpy as jnp
from jax import lax

C = 69
HID = 256
WINDOW = 5
LON = 256
NT = 32
NH = 64


def steps_of(stream_key, extent, cuts, smallest, high):
    def one(dim, shards_of):
        steps = jax.random.uniform(jax.random.fold_in(jax.random.fold_in(stream_key, 6), dim), (shards_of,), jnp.float32, smallest / len(cuts), high / len(cuts))
        return jnp.repeat(jnp.exp(steps), extent[dim] // shards_of).reshape((-1,) + (1,) * (len(extent) - dim - 1))

    loudness = one(*cuts[0])
    for cut in cuts[1:]:
        loudness = loudness * one(*cut)
    return loudness


def noise(key, dims, spread, bound, cuts=(), held_as=jnp.bfloat16):
    values = jax.random.normal(key, dims, jnp.float32) * spread
    if len(cuts) > 0:
        values = steps_of(key, dims, cuts, -0.22, 0.18) * values
    return jnp.clip(values, min=-bound, max=bound).astype(held_as)


def setup_inputs(seed: int = 0) -> dict:
    keys = jax.random.split(jax.random.key(seed), 7)
    states = noise(keys[0], (NT, C, NH, LON), 1.0, 6.0, ((0, 16), (2, 16)), jnp.float32)
    observed = noise(keys[1], (NT, C, NH, LON), 1.0, 6.0, ((0, 16), (2, 16)), jnp.float32)
    conv_in = noise(keys[2], (3, 3, HID, WINDOW * C), (9 * WINDOW * C) ** -0.5, 0.109375)
    bias_in = noise(keys[3], (HID,), 0.5, 3.0, (), jnp.float32)
    conv_out = noise(keys[4], (3, 3, C, HID), (9 * HID) ** -0.5, 0.125)
    bias_out = noise(keys[5], (C,), 0.5, 3.0, (), jnp.float32)
    return dict(states=states, observed=observed, conv_in=conv_in, bias_in=bias_in, conv_out=conv_out, bias_out=bias_out)


def convolve(padded, weights):
    rows = padded.shape[1] - 2
    channels = padded.shape[0]
    total = None
    for j in range(3):
        moved = jnp.roll(padded, 1 - j, axis=2)
        for i in range(3):
            band = moved[:, i:i + rows, :]
            term = jnp.dot(weights[i, j], band.reshape(channels, -1), preferred_element_type=jnp.float32)
            total = term if total is None else total + term
    return total.reshape(weights.shape[2], rows, padded.shape[2])


def pad_rows(field):
    return jnp.pad(field, ((0, 0), (1, 1), (0, 0)))


def flipped(weights):
    return jnp.transpose(weights[::-1, ::-1], (0, 1, 3, 2))


def silu_slope(value):
    sig = jax.nn.sigmoid(value)
    return sig * (1.0 + value * (1.0 - sig))


def reference(states, observed, conv_in, bias_in, conv_out, bias_out):
    total = states.shape[0]
    chans = states.shape[1]
    height = states.shape[2]
    width = states.shape[3]
    cast = states.astype(jnp.bfloat16)
    back_in = flipped(conv_in)
    back_out = flipped(conv_out)

    def one_window(index):
        picks = ((index + jnp.arange(WINDOW, dtype=jnp.int32) - 2) % total).astype(jnp.int32)
        stacked = jnp.take(cast, picks, axis=0).reshape(WINDOW * chans, height, width)
        pre = convolve(pad_rows(stacked), conv_in) + bias_in[:, None, None]
        act = jax.nn.silu(pre).astype(jnp.bfloat16)
        score = convolve(pad_rows(act), conv_out) + bias_out[:, None, None]
        target = lax.dynamic_index_in_dim(observed, index, 0, False)
        resid = (score - target).astype(jnp.bfloat16)
        grad_act = convolve(pad_rows(resid), back_out)
        grad_pre = (grad_act * silu_slope(pre)).astype(jnp.bfloat16)
        grad_window = convolve(pad_rows(grad_pre), back_in)
        return score, grad_window.reshape(WINDOW, chans, height, width)

    scores, grads = lax.map(one_window, jnp.arange(total, dtype=jnp.int32))
    guidance = jnp.roll(grads[:, 0], -2, axis=0)
    for k in range(1, WINDOW):
        guidance = guidance + jnp.roll(grads[:, k], k - 2, axis=0)
    return scores, guidance
```

```python
import jax
import jax.numpy as jnp
from jax import lax
from jax.experimental import pallas as pl
from jax.experimental.pallas import tpu as pltpu
from jax.sharding import PartitionSpec as P

MESH = pl.DeviceIdType.MESH
F32 = jnp.float32
BF16 = jnp.bfloat16
C = 69
HID = 256
WINDOW = 5
LON = 256
ROWS = 4
OWN = 2
SPAN = OWN + WINDOW - 1
MAIN = 64
TAIL = 8
STACK = 3 * (MAIN + TAIL)
ZROWS = 224
CHUNK = 2 * MAIN + 2 * TAIL
EDGE = MAIN + 2 * TAIL


def dot(a, b):
    return jnp.dot(a, b, preferred_element_type=F32)


def parts(x):
    tail = jnp.concatenate([x[MAIN:], jnp.zeros((MAIN + TAIL - C, x.shape[1]), F32)], axis=0)
    return x[:MAIN], tail


def left(x):
    return pltpu.roll(x, LON - 1, axis=1)


def right(x):
    return pltpu.roll(x, 1, axis=1)


def stack_into(ref, main, tail, first, last):
    ref[0:64, :] = first(main)
    ref[64:128, :] = main
    ref[128:192, :] = last(main)
    tails = jnp.concatenate([first(tail), tail, last(tail), jnp.zeros((TAIL, LON), F32)], axis=0)
    ref[192:224, :] = tails.astype(BF16)


def combine(z, first, last):
    main = first(z[0:64]) + z[64:128] + last(z[128:192])
    tail = first(z[192:200]) + z[200:208] + last(z[208:216])
    return main, tail


def kernel(
    states, observed, conv_in, bias_in, conv_out, bias_out, scores_out, guidance_out,
    st, ob, wi, wo, w4, w1, w2, w2t, bi, bo, sbuf, rbuf, hb, xs, pre, slope, act, sp, rp, kc, sc,
    rs, gp, sg, rg, own, so, go,
    local, tm_send, tm_recv, lat_send, lat_recv, x2_send, x2_recv, x3_send, x3_recv, g_send, g_recv,
):
    m = lax.axis_index("tm")
    l = lax.axis_index("lat")
    count_m = lax.axis_size("tm")
    count_l = lax.axis_size("lat")
    nxt = lax.rem(m + 1, count_m)
    prv = lax.rem(m + count_m - 1, count_m)
    has_up = l > 0
    has_down = l < count_l - 1

    load_st = pltpu.make_async_copy(states, st, local.at[0])
    load_wi = pltpu.make_async_copy(conv_in, wi, local.at[1])
    load_wo = pltpu.make_async_copy(conv_out, wo, local.at[2])
    load_ob = pltpu.make_async_copy(observed, ob, local.at[3])
    load_st.start()
    load_wi.start()
    load_wo.start()
    load_ob.start()

    barrier = pltpu.get_barrier_semaphore()
    pl.semaphore_signal(barrier, inc=1, device_id=(nxt, l), device_id_type=MESH)
    pl.semaphore_signal(barrier, inc=1, device_id=(prv, l), device_id_type=MESH)

    @pl.when(has_up)
    def _():
        pl.semaphore_signal(barrier, inc=1, device_id=(m, l - 1), device_id_type=MESH)

    @pl.when(has_down)
    def _():
        pl.semaphore_signal(barrier, inc=1, device_id=(m, l + 1), device_id_type=MESH)

    def remote(src, dst, send, recv, where):
        return pltpu.make_async_remote_copy(
            src_ref=src, dst_ref=dst, send_sem=send, recv_sem=recv, device_id=where, device_id_type=MESH
        )

    def tm_copy(d, s, g):
        where = (nxt, l) if d == 0 else (prv, l)
        return remote(sbuf.at[s, g], rbuf.at[d, s, g], tm_send.at[d, s, g], tm_recv.at[d, s, g], where)

    def lat_copy(d, e, chunk):
        if d == 0:
            return remote(chunk.at[pl.ds(MAIN, EDGE)], hb.at[0, e], lat_send.at[0, e], lat_recv.at[0, e], (m, l + 1))
        return remote(chunk.at[pl.ds(0, EDGE)], hb.at[1, e], lat_send.at[1, e], lat_recv.at[1, e], (m, l - 1))

    def chunk_of(e, g):
        if e < OWN:
            return rbuf.at[0, e, g]
        if e < 2 * OWN:
            return sbuf.at[e - OWN, g]
        return rbuf.at[1, e - 2 * OWN, g]

    def lat_start(e):
        @pl.when(has_down)
        def _():
            lat_copy(0, e, chunk_of(e, 0)).start()

        @pl.when(has_up)
        def _():
            lat_copy(1, e, chunk_of(e, 0)).start()

    def x2_copy(d):
        where = (m, l + 1) if d == 0 else (m, l - 1)
        return remote(sp.at[d], rp.at[d], x2_send.at[d], x2_recv.at[d], where)

    def x3_copy(d):
        if d == 0:
            return remote(gp.at[4], gp.at[0], x3_send.at[0], x3_recv.at[0], (m, l + 1))
        return remote(gp.at[1], gp.at[5], x3_send.at[1], x3_recv.at[1], (m, l - 1))

    def g_copy(d, r):
        where = (nxt, l) if d == 0 else (prv, l)
        return remote(sg.at[d, r], rg.at[d, r], g_send.at[d, r], g_recv.at[d, r], where)

    load_st.wait()
    for g, (a, b) in enumerate(((0, 3), (1, 2))):
        for s in range(OWN):
            main_a, tail_a = parts(st[s, :, a, :])
            main_b, tail_b = parts(st[s, :, b, :])
            sbuf[s, g, 0:64, :] = main_a.astype(BF16)
            sbuf[s, g, 64:80, :] = jnp.concatenate([tail_a, tail_b], axis=0).astype(BF16)
            sbuf[s, g, 80:144, :] = main_b.astype(BF16)
        if g == 0:
            pl.semaphore_wait(barrier, 2 + has_up.astype(jnp.int32) + has_down.astype(jnp.int32))

        tm_copy(0, 1, g).start()
        tm_copy(1, 0, g).start()
        tm_copy(0, 0, g).start()
        tm_copy(1, 1, g).start()
        if g == 0:
            for s in range(OWN):
                lat_start(OWN + s)

    def zero_pads(n, carry):
        xs[n // SPAN, lax.rem(n, SPAN), ZROWS:256, :] = jnp.zeros((256 - ZROWS, LON), BF16)
        return carry

    lax.fori_loop(0, (ROWS + 2) * SPAN, zero_pads, 0)
    for rho in range(ROWS + 2):
        for t in range(OWN):
            rs[rho, t, ZROWS:256, :] = jnp.zeros((256 - ZROWS, LON), BF16)

    def zero_halo(rho):
        def one(e, carry):
            xs[rho, e, 0:ZROWS, :] = jnp.zeros((ZROWS, LON), BF16)
            return carry

        lax.fori_loop(0, SPAN, one, 0)
        for t in range(OWN):
            rs[rho, t, 0:ZROWS, :] = jnp.zeros((ZROWS, LON), BF16)
            gp[rho, t] = jnp.zeros((HID, LON), BF16)

    @pl.when(jnp.logical_not(has_up))
    def _():
        zero_halo(0)

    @pl.when(jnp.logical_not(has_down))
    def _():
        zero_halo(ROWS + 1)

    bi[...] = jnp.broadcast_to(bias_in[...][None, :], (HID, HID)).T
    row = jnp.concatenate([bias_out[...][None, :], jnp.zeros((1, 128 - C), F32)], axis=1)
    column = jnp.broadcast_to(row, (128, 128)).T
    bo[...] = jnp.concatenate([column[: MAIN + TAIL], column[: MAIN + TAIL]], axis=1)

    load_wi.wait()

    def weights(i, carry):
        for k in range(WINDOW):
            tails = []
            for j in range(3):
                low = (C * k) // 16 * 16
                high = min((C * k + C + 15) // 16 * 16, WINDOW * C)
                piece = wi[i, j, low:high, :].astype(F32)[C * k - low : C * k - low + C]
                main, tail = parts(piece)
                w4[i, k, 64 * j : 64 * j + 64, :] = main.astype(BF16)
                tails.append(tail)
            tails.append(jnp.zeros((MAIN - 3 * TAIL, HID), F32))
            w4[i, k, 192:256, :] = jnp.concatenate(tails, axis=0).astype(BF16)
            w1[i, k] = w4[i, k].T
        return carry

    lax.fori_loop(0, 3, weights, 0)
    load_wo.wait()
    for i in range(3):
        tails = []
        for j in range(3):
            main, tail = parts(wo[i, j].astype(F32))
            w2[i, 64 * j : 64 * j + 64, :] = main.astype(BF16)
            tails.append(tail)
        tails.append(jnp.zeros((MAIN - 3 * TAIL, HID), F32))
        w2[i, 192:256, :] = jnp.concatenate(tails, axis=0).astype(BF16)
        w2t[i] = w2[i].T

    def stack_chunk(e, g):
        chunk = chunk_of(e, g)
        tails = chunk[64:80, :].astype(F32)
        a, b = ((0, 3), (1, 2))[g]
        stack_into(xs.at[a + 1, e], chunk[0:64, :], tails[0:8], right, left)
        stack_into(xs.at[b + 1, e], chunk[80:144, :], tails[8:16], right, left)

    def stack_halo(e):
        @pl.when(has_up)
        def _():
            lat_copy(0, e, chunk_of(e, 0)).wait_recv()
            stack_into(xs.at[0, e], hb[0, e, 16:80, :], hb[0, e, 0:16, :].astype(F32)[8:16], right, left)

        @pl.when(has_down)
        def _():
            lat_copy(1, e, chunk_of(e, 0)).wait_recv()
            stack_into(xs.at[5, e], hb[1, e, 0:64, :], hb[1, e, 64:80, :].astype(F32)[0:8], right, left)

    for s in range(OWN):
        stack_chunk(OWN + s, 0)
        stack_chunk(OWN + s, 1)
    for s in range(OWN):
        stack_halo(OWN + s)

    def conv_states(t, r, total, picks):
        for e in picks:
            for i in range(3):
                total = total + dot(w1[i, e - t], xs[r + i, e])
        return total

    def phase_own(n, carry):
        t = lax.rem(n, OWN)
        r = n // OWN
        pre[t, r] = conv_states(t, r, bi[...], (2, 3))
        return carry

    lax.fori_loop(0, OWN * ROWS, phase_own, 0)

    tm_copy(0, 1, 0).wait_recv()
    lat_start(1)
    tm_copy(1, 0, 0).wait_recv()
    lat_start(4)
    stack_chunk(1, 0)
    stack_chunk(4, 0)
    tm_copy(0, 0, 0).wait_recv()
    lat_start(0)
    tm_copy(1, 1, 0).wait_recv()
    lat_start(5)
    stack_chunk(0, 0)
    stack_chunk(5, 0)
    tm_copy(0, 1, 1).wait_recv()
    tm_copy(1, 0, 1).wait_recv()
    stack_chunk(1, 1)
    stack_chunk(4, 1)
    stack_halo(1)
    stack_halo(4)

    def phase_near(n, carry):
        t = lax.rem(n, OWN)
        r = n // OWN
        pre[t, r] = conv_states(t, r, pre[t, r], (1, 4))
        return carry

    lax.fori_loop(0, OWN * ROWS, phase_near, 0)
    tm_copy(0, 0, 1).wait_recv()
    tm_copy(1, 1, 1).wait_recv()
    stack_chunk(0, 1)
    stack_chunk(5, 1)
    stack_halo(0)
    stack_halo(5)

    def phase_far(n, carry):
        t = lax.rem(n, OWN)
        r = n // OWN
        v = pre[t, r]
        for i in range(3):
            v = v + dot(w1[i, 4 * t], xs[r + i, 5 * t])
        sig = 0.5 + 0.5 * jnp.tanh(0.5 * v)
        act[r, t] = (v * sig).astype(BF16)
        slope[r, t] = sig * (1.0 + v * (1.0 - sig))
        return carry

    lax.fori_loop(0, OWN * ROWS, phase_far, 0)

    load_ob.wait()

    def score_terms(t, pairs):
        z = None
        for i, r in pairs:
            term = dot(w2[i, 0:ZROWS, :], act[r, t])
            z = term if z is None else z + term
        return combine(z, right, left)

    def pack_score(t, d, kind, main, tail):
        q = 2 * kind + t
        sp[d, 64 * q : 64 * q + 64, :] = main.astype(BF16)
        return tail

    for d, given, kept, r in ((0, ((0, 3),), ((0, 2), (1, 3)), 3), (1, ((2, 0),), ((1, 0), (2, 1)), 0)):
        tails = [None] * 4
        for t in range(OWN):
            main, tail = score_terms(t, given)
            kc[d, t, 0:64, :] = main
            kc[d, t, 64:72, :] = tail
            tails[t] = pack_score(t, d, 0, main, tail)
            main, tail = score_terms(t, kept)
            main = main + bo[0:64, :]
            tail = tail + bo[64:72, :]
            sc[r, t, 0:64, :] = main
            sc[r, t, 64:72, :] = tail
            seen_main, seen_tail = parts(ob[t, :, r, :])
            tails[2 + t] = pack_score(t, d, 1, main - seen_main, tail - seen_tail)
        sp[d, 256:288, :] = jnp.concatenate(tails, axis=0).astype(BF16)

        @pl.when(has_down if d == 0 else has_up)
        def _():
            x2_copy(d).start()

    def finish_row(t, r, main, tail):
        so[t, :, r, :] = jnp.concatenate([main, tail[: C - MAIN]], axis=0)
        seen_main, seen_tail = parts(ob[t, :, r, :])
        stack_into(rs.at[r + 1, t], (main - seen_main).astype(BF16), tail - seen_tail, left, right)

    for t in range(OWN):
        for r in (1, 2):
            main, tail = score_terms(t, tuple((i, r + i - 1) for i in range(3)))
            finish_row(t, r, main + bo[0:64, :], tail + bo[64:72, :])

    for d, r, halo, present in ((0, 0, 0, has_up), (1, 3, 5, has_down)):
        @pl.when(present)
        def _():
            x2_copy(d).wait_recv()
            tails = rp[d, 256:288, :].astype(F32)
            for t in range(OWN):
                sc[r, t, 0:64, :] += rp[d, 64 * t : 64 * t + 64, :].astype(F32)
                sc[r, t, 64:72, :] += tails[8 * t : 8 * t + 8]
                q = 2 + t
                main = kc[1 - d, t, 0:64, :] + rp[d, 64 * q : 64 * q + 64, :].astype(F32)
                tail = kc[1 - d, t, 64:72, :] + tails[8 * q : 8 * q + 8]
                stack_into(rs.at[halo, t], main.astype(BF16), tail, left, right)

    for t in range(OWN):
        for r in (0, 3):
            finish_row(t, r, sc[r, t, 0:64, :], sc[r, t, 64:72, :])

    store_scores = pltpu.make_async_copy(so, scores_out, local.at[4])
    store_scores.start()

    def grad_hidden(t, r):
        total = None
        for i in range(3):
            term = dot(w2t[i], rs[r + 2 - i, t])
            total = term if total is None else total + term
        gp[r + 1, t] = (total * slope[r, t]).astype(BF16)

    def hidden_outer(n, carry):
        grad_hidden(lax.rem(n, OWN), 3 * (n // OWN))
        return carry

    def hidden_inner(n, carry):
        grad_hidden(lax.rem(n, OWN), 1 + n // OWN)
        return carry

    lax.fori_loop(0, 2 * OWN, hidden_outer, 0)

    @pl.when(has_down)
    def _():
        x3_copy(0).start()

    @pl.when(has_up)
    def _():
        x3_copy(1).start()

    lax.fori_loop(0, 2 * OWN, hidden_inner, 0)

    def grad_state(e, r):
        z = None
        for t in range(OWN):
            k = e - t
            if 0 <= k < WINDOW:
                for i in range(3):
                    term = dot(w4[i, k, 0:ZROWS, :], gp[r + 2 - i, t])
                    z = term if z is None else z + term
        return combine(z, left, right)

    def send_row(r):
        for d, e in ((1, 0), (0, 4)):
            main_a, tail_a = grad_state(e, r)
            main_b, tail_b = grad_state(e + 1, r)
            sg[d, r, 0:64, :] = main_a.astype(BF16)
            sg[d, r, 64:80, :] = jnp.concatenate([tail_a, tail_b], axis=0).astype(BF16)
            sg[d, r, 80:144, :] = main_b.astype(BF16)
            g_copy(d, r).start()

    def own_row(r):
        for s in range(OWN):
            main, tail = grad_state(OWN + s, r)
            own[r, s, 0:64, :] = main
            own[r, s, 64:72, :] = tail

    def send_inner(n, carry):
        send_row(1 + n)
        return carry

    def own_inner(n, carry):
        own_row(1 + n)
        return carry

    def send_outer(n, carry):
        send_row(3 * n)
        return carry

    def own_outer(n, carry):
        own_row(3 * n)
        return carry

    lax.fori_loop(0, 2, send_inner, 0)
    lax.fori_loop(0, 2, own_inner, 0)

    @pl.when(has_up)
    def _():
        x3_copy(0).wait_recv()

    @pl.when(has_down)
    def _():
        x3_copy(1).wait_recv()

    lax.fori_loop(0, 2, send_outer, 0)
    lax.fori_loop(0, 2, own_outer, 0)

    for r in (1, 2, 0, 3):
        g_copy(0, r).wait_recv()
        g_copy(1, r).wait_recv()
        tails = rg[0, r, 64:80, :].astype(F32) + rg[1, r, 64:80, :].astype(F32)
        for s in range(OWN):
            low = 80 * s
            main = own[r, s, 0:64, :] + rg[0, r, low : low + 64, :].astype(F32) + rg[1, r, low : low + 64, :].astype(F32)
            tail = own[r, s, 64:72, :] + tails[8 * s : 8 * s + 8]
            go[s, :, r, :] = jnp.concatenate([main, tail[: C - MAIN]], axis=0)
    store_guidance = pltpu.make_async_copy(go, guidance_out, local.at[5])
    store_guidance.start()

    for d in range(2):
        for s in range(OWN):
            for g in range(2):
                tm_copy(d, s, g).wait_send()
        for r in range(ROWS):
            g_copy(d, r).wait_send()

        @pl.when(has_down if d == 0 else has_up)
        def _():
            for e in range(SPAN):
                lat_copy(d, e, chunk_of(e, 0)).wait_send()
            x2_copy(d).wait_send()
            x3_copy(d).wait_send()

    store_scores.wait()
    store_guidance.wait()


def solution(mesh):
    whole = P("tm", None, "lat", None)

    def step(states, observed, conv_in, bias_in, conv_out, bias_out):
        shape = states.shape
        dma = pltpu.SemaphoreType.DMA
        any_space = pl.BlockSpec(memory_space=pl.ANY)
        vmem = pl.BlockSpec(memory_space=pltpu.VMEM)
        return pl.pallas_call(
            kernel,
            out_shape=(jax.ShapeDtypeStruct(shape, F32), jax.ShapeDtypeStruct(shape, F32)),
            in_specs=[any_space, any_space, any_space, vmem, any_space, vmem],
            out_specs=(any_space, any_space),
            scratch_shapes=[
                pltpu.VMEM(shape, F32),
                pltpu.VMEM(shape, F32),
                pltpu.VMEM((3, 3, WINDOW * C, HID), BF16),
                pltpu.VMEM((3, 3, C, HID), BF16),
                pltpu.VMEM((3, WINDOW, 256, HID), BF16),
                pltpu.VMEM((3, WINDOW, HID, 256), BF16),
                pltpu.VMEM((3, 256, HID), BF16),
                pltpu.VMEM((3, HID, 256), BF16),
                pltpu.VMEM((HID, LON), F32),
                pltpu.VMEM((MAIN + TAIL, LON), F32),
                pltpu.VMEM((OWN, 2, CHUNK, LON), BF16),
                pltpu.VMEM((2, OWN, 2, CHUNK, LON), BF16),
                pltpu.VMEM((2, SPAN, EDGE, LON), BF16),
                pltpu.VMEM((ROWS + 2, SPAN, 256, LON), BF16),
                pltpu.VMEM((OWN, ROWS, HID, LON), F32),
                pltpu.VMEM((ROWS, OWN, HID, LON), F32),
                pltpu.VMEM((ROWS, OWN, HID, LON), BF16),
                pltpu.VMEM((2, 4 * (MAIN + TAIL), LON), BF16),
                pltpu.VMEM((2, 4 * (MAIN + TAIL), LON), BF16),
                pltpu.VMEM((2, OWN, MAIN + TAIL, LON), F32),
                pltpu.VMEM((ROWS, OWN, MAIN + TAIL, LON), F32),
                pltpu.VMEM((ROWS + 2, OWN, 256, LON), BF16),
                pltpu.VMEM((ROWS + 2, OWN, HID, LON), BF16),
                pltpu.VMEM((2, ROWS, CHUNK, LON), BF16),
                pltpu.VMEM((2, ROWS, CHUNK, LON), BF16),
                pltpu.VMEM((ROWS, OWN, MAIN + TAIL, LON), F32),
                pltpu.VMEM(shape, F32),
                pltpu.VMEM(shape, F32),
                dma((6,)),
                dma((2, OWN, 2)),
                dma((2, OWN, 2)),
                dma((2, SPAN)),
                dma((2, SPAN)),
                dma((2,)),
                dma((2,)),
                dma((2,)),
                dma((2,)),
                dma((2, ROWS)),
                dma((2, ROWS)),
            ],
            compiler_params=pltpu.CompilerParams(
                collective_id=0, has_side_effects=True, vmem_limit_bytes=60 * 1024 * 1024
            ),
        )(states, observed, jnp.transpose(conv_in, (0, 1, 3, 2)), bias_in, conv_out, bias_out)

    sharded = jax.shard_map(
        step, mesh=mesh, in_specs=(whole, whole, P(), P(), P(), P()), out_specs=(whole, whole), check_vma=False
    )

    def run(*args):
        with jax.sharding.use_abstract_mesh(mesh.abstract_mesh):
            return sharded(*args)

    return run
```

```python
import jax
import jax.numpy as jnp
from jax import lax
from jax.experimental import pallas as pl
from jax.experimental.pallas import tpu as pltpu
from jax.sharding import PartitionSpec as P

MESH = pl.DeviceIdType.MESH
F32 = jnp.float32
BF16 = jnp.bfloat16
C = 69
HID = 256
WINDOW = 5
LON = 256
ROWS = 4
OWN = 2
SPAN = OWN + WINDOW - 1
MAIN = 64
TAIL = 8
STACK = 3 * (MAIN + TAIL)
ZROWS = 224
CHUNK = 2 * MAIN + 2 * TAIL
EDGE = MAIN + 2 * TAIL


def dot(a, b):
    return jnp.dot(a, b, preferred_element_type=F32)


def parts(x):
    tail = jnp.concatenate([x[MAIN:], jnp.zeros((MAIN + TAIL - C, x.shape[1]), F32)], axis=0)
    return x[:MAIN], tail


def row_of(ref, s, r):
    return jnp.concatenate([ref[s, pl.ds(ROWS * h + r, C, stride=2 * ROWS), :] for h in range(2)], axis=1)


def put_row(ref, s, r, main, tail):
    for h in range(2):
        lanes = slice(128 * h, 128 * h + 128)
        ref[s, pl.ds(ROWS * h + r, MAIN, stride=2 * ROWS), :] = main[:, lanes]
        ref[s, pl.ds(2 * ROWS * MAIN + ROWS * h + r, C - MAIN, stride=2 * ROWS), :] = tail[: C - MAIN, lanes]


def left(x):
    return pltpu.roll(x, LON - 1, axis=1)


def right(x):
    return pltpu.roll(x, 1, axis=1)


def stack_into(ref, main, tail, first, last):
    ref[0:64, :] = first(main)
    ref[64:128, :] = main
    ref[128:192, :] = last(main)
    tails = jnp.concatenate([first(tail), tail, last(tail), jnp.zeros((TAIL, LON), F32)], axis=0)
    ref[192:224, :] = tails.astype(BF16)


def combine(z, first, last):
    main = first(z[0:64]) + z[64:128] + last(z[128:192])
    tail = first(z[192:200]) + z[200:208] + last(z[208:216])
    return main, tail


def kernel(
    states, observed, conv_in, bias_in, conv_out, bias_out, so, go,
    st, ob, wi, wo, w4, w1, w2, w2t, bi, bo, sbuf, rbuf, hb, xs, pre, slope, act, sp, rp, kc, sc,
    rs, gp, sg, rg, own,
    local, tm_send, tm_recv, lat_send, lat_recv, x2_send, x2_recv, x3_send, x3_recv, g_send, g_recv,
):
    m = lax.axis_index("tm")
    l = lax.axis_index("lat")
    count_m = lax.axis_size("tm")
    count_l = lax.axis_size("lat")
    nxt = lax.rem(m + 1, count_m)
    prv = lax.rem(m + count_m - 1, count_m)
    has_up = l > 0
    has_down = l < count_l - 1

    load_st = pltpu.make_async_copy(states, st, local.at[0])
    load_wi = pltpu.make_async_copy(conv_in, wi, local.at[1])
    load_wo = pltpu.make_async_copy(conv_out, wo, local.at[2])
    load_ob = pltpu.make_async_copy(observed, ob, local.at[3])
    load_st.start()
    load_wi.start()
    load_wo.start()
    load_ob.start()

    barrier = pltpu.get_barrier_semaphore()
    pl.semaphore_signal(barrier, inc=1, device_id=(nxt, l), device_id_type=MESH)
    pl.semaphore_signal(barrier, inc=1, device_id=(prv, l), device_id_type=MESH)

    @pl.when(has_up)
    def _():
        pl.semaphore_signal(barrier, inc=1, device_id=(m, l - 1), device_id_type=MESH)

    @pl.when(has_down)
    def _():
        pl.semaphore_signal(barrier, inc=1, device_id=(m, l + 1), device_id_type=MESH)

    def remote(src, dst, send, recv, where):
        return pltpu.make_async_remote_copy(
            src_ref=src, dst_ref=dst, send_sem=send, recv_sem=recv, device_id=where, device_id_type=MESH
        )

    def tm_copy(d, s, g):
        where = (nxt, l) if d == 0 else (prv, l)
        return remote(sbuf.at[s, g], rbuf.at[d, s, g], tm_send.at[d, s, g], tm_recv.at[d, s, g], where)

    def lat_copy(d, e, chunk):
        if d == 0:
            return remote(chunk.at[pl.ds(MAIN, EDGE)], hb.at[0, e], lat_send.at[0, e], lat_recv.at[0, e], (m, l + 1))
        return remote(chunk.at[pl.ds(0, EDGE)], hb.at[1, e], lat_send.at[1, e], lat_recv.at[1, e], (m, l - 1))

    def chunk_of(e, g):
        if e < OWN:
            return rbuf.at[0, e, g]
        if e < 2 * OWN:
            return sbuf.at[e - OWN, g]
        return rbuf.at[1, e - 2 * OWN, g]

    def lat_start(e):
        @pl.when(has_down)
        def _():
            lat_copy(0, e, chunk_of(e, 0)).start()

        @pl.when(has_up)
        def _():
            lat_copy(1, e, chunk_of(e, 0)).start()

    def x2_copy(d):
        where = (m, l + 1) if d == 0 else (m, l - 1)
        return remote(sp.at[d], rp.at[d], x2_send.at[d], x2_recv.at[d], where)

    def x3_copy(d):
        if d == 0:
            return remote(gp.at[4], gp.at[0], x3_send.at[0], x3_recv.at[0], (m, l + 1))
        return remote(gp.at[1], gp.at[5], x3_send.at[1], x3_recv.at[1], (m, l - 1))

    def g_copy(d, r):
        where = (nxt, l) if d == 0 else (prv, l)
        return remote(sg.at[d, r], rg.at[d, r], g_send.at[d, r], g_recv.at[d, r], where)

    load_st.wait()
    for g, (a, b) in enumerate(((0, 3), (1, 2))):
        for s in range(OWN):
            main_a, tail_a = parts(row_of(st, s, a))
            main_b, tail_b = parts(row_of(st, s, b))
            sbuf[s, g, 0:64, :] = main_a.astype(BF16)
            sbuf[s, g, 64:80, :] = jnp.concatenate([tail_a, tail_b], axis=0).astype(BF16)
            sbuf[s, g, 80:144, :] = main_b.astype(BF16)
        if g == 0:
            pl.semaphore_wait(barrier, 2 + has_up.astype(jnp.int32) + has_down.astype(jnp.int32))

        tm_copy(0, 1, g).start()
        tm_copy(1, 0, g).start()
        tm_copy(0, 0, g).start()
        tm_copy(1, 1, g).start()
        if g == 0:
            for s in range(OWN):
                lat_start(OWN + s)

    def zero_pads(n, carry):
        xs[n // SPAN, lax.rem(n, SPAN), ZROWS:256, :] = jnp.zeros((256 - ZROWS, LON), BF16)
        return carry

    lax.fori_loop(0, (ROWS + 2) * SPAN, zero_pads, 0)
    for rho in range(ROWS + 2):
        for t in range(OWN):
            rs[rho, t, ZROWS:256, :] = jnp.zeros((256 - ZROWS, LON), BF16)

    def zero_halo(rho):
        def one(e, carry):
            xs[rho, e, 0:ZROWS, :] = jnp.zeros((ZROWS, LON), BF16)
            return carry

        lax.fori_loop(0, SPAN, one, 0)
        for t in range(OWN):
            rs[rho, t, 0:ZROWS, :] = jnp.zeros((ZROWS, LON), BF16)
            gp[rho, t] = jnp.zeros((HID, LON), BF16)

    @pl.when(jnp.logical_not(has_up))
    def _():
        zero_halo(0)

    @pl.when(jnp.logical_not(has_down))
    def _():
        zero_halo(ROWS + 1)

    bi[...] = jnp.broadcast_to(bias_in[...][None, :], (HID, HID)).T
    row = jnp.concatenate([bias_out[...][None, :], jnp.zeros((1, 128 - C), F32)], axis=1)
    column = jnp.broadcast_to(row, (128, 128)).T
    bo[...] = jnp.concatenate([column[: MAIN + TAIL], column[: MAIN + TAIL]], axis=1)

    load_wi.wait()

    def weights(i, carry):
        for k in range(WINDOW):
            tails = []
            for j in range(3):
                low = (C * k) // 16 * 16
                high = min((C * k + C + 15) // 16 * 16, WINDOW * C)
                piece = wi[i, j, low:high, :].astype(F32)[C * k - low : C * k - low + C]
                main, tail = parts(piece)
                w4[i, k, 64 * j : 64 * j + 64, :] = main.astype(BF16)
                tails.append(tail)
            tails.append(jnp.zeros((MAIN - 3 * TAIL, HID), F32))
            w4[i, k, 192:256, :] = jnp.concatenate(tails, axis=0).astype(BF16)
            w1[i, k] = w4[i, k].T
        return carry

    lax.fori_loop(0, 3, weights, 0)
    load_wo.wait()
    for i in range(3):
        tails = []
        for j in range(3):
            main, tail = parts(wo[i, j].astype(F32))
            w2[i, 64 * j : 64 * j + 64, :] = main.astype(BF16)
            tails.append(tail)
        tails.append(jnp.zeros((MAIN - 3 * TAIL, HID), F32))
        w2[i, 192:256, :] = jnp.concatenate(tails, axis=0).astype(BF16)
        w2t[i] = w2[i].T

    def stack_chunk(e, g):
        chunk = chunk_of(e, g)
        tails = chunk[64:80, :].astype(F32)
        a, b = ((0, 3), (1, 2))[g]
        stack_into(xs.at[a + 1, e], chunk[0:64, :], tails[0:8], right, left)
        stack_into(xs.at[b + 1, e], chunk[80:144, :], tails[8:16], right, left)

    def stack_halo(e):
        @pl.when(has_up)
        def _():
            lat_copy(0, e, chunk_of(e, 0)).wait_recv()
            stack_into(xs.at[0, e], hb[0, e, 16:80, :], hb[0, e, 0:16, :].astype(F32)[8:16], right, left)

        @pl.when(has_down)
        def _():
            lat_copy(1, e, chunk_of(e, 0)).wait_recv()
            stack_into(xs.at[5, e], hb[1, e, 0:64, :], hb[1, e, 64:80, :].astype(F32)[0:8], right, left)

    for s in range(OWN):
        stack_chunk(OWN + s, 0)
        stack_chunk(OWN + s, 1)
    for s in range(OWN):
        stack_halo(OWN + s)

    def conv_states(t, r, total, picks):
        for e in picks:
            for i in range(3):
                total = total + dot(w1[i, e - t], xs[r + i, e])
        return total

    def phase_own(n, carry):
        t = lax.rem(n, OWN)
        r = n // OWN
        pre[t, r] = conv_states(t, r, bi[...], (2, 3))
        return carry

    lax.fori_loop(0, OWN * ROWS, phase_own, 0, unroll=True)

    tm_copy(0, 1, 0).wait_recv()
    lat_start(1)
    tm_copy(1, 0, 0).wait_recv()
    lat_start(4)
    stack_chunk(1, 0)
    stack_chunk(4, 0)
    tm_copy(0, 0, 0).wait_recv()
    lat_start(0)
    tm_copy(1, 1, 0).wait_recv()
    lat_start(5)
    stack_chunk(0, 0)
    stack_chunk(5, 0)
    tm_copy(0, 1, 1).wait_recv()
    tm_copy(1, 0, 1).wait_recv()
    stack_chunk(1, 1)
    stack_chunk(4, 1)
    stack_halo(1)
    stack_halo(4)

    def phase_near(n, carry):
        t = lax.rem(n, OWN)
        r = n // OWN
        pre[t, r] = conv_states(t, r, pre[t, r], (1, 4))
        return carry

    lax.fori_loop(0, OWN * ROWS, phase_near, 0, unroll=True)
    tm_copy(0, 0, 1).wait_recv()
    tm_copy(1, 1, 1).wait_recv()
    stack_chunk(0, 1)
    stack_chunk(5, 1)
    stack_halo(0)
    stack_halo(5)

    def phase_far(n, carry):
        t = lax.rem(n, OWN)
        r = n // OWN
        v = pre[t, r]
        for i in range(3):
            v = v + dot(w1[i, 4 * t], xs[r + i, 5 * t])
        sig = 0.5 + 0.5 * jnp.tanh(0.5 * v)
        act[r, t] = (v * sig).astype(BF16)
        slope[r, t] = sig * (1.0 + v * (1.0 - sig))
        return carry

    lax.fori_loop(0, OWN * ROWS, phase_far, 0, unroll=True)

    load_ob.wait()

    def score_terms(t, pairs):
        z = None
        for i, r in pairs:
            term = dot(w2[i, 0:ZROWS, :], act[r, t])
            z = term if z is None else z + term
        return combine(z, right, left)

    def pack_score(t, d, kind, main, tail):
        q = 2 * kind + t
        sp[d, 64 * q : 64 * q + 64, :] = main.astype(BF16)
        return tail

    for d, given, kept, r in ((0, ((0, 3),), ((0, 2), (1, 3)), 3), (1, ((2, 0),), ((1, 0), (2, 1)), 0)):
        tails = [None] * 4
        for t in range(OWN):
            main, tail = score_terms(t, given)
            kc[d, t, 0:64, :] = main
            kc[d, t, 64:72, :] = tail
            tails[t] = pack_score(t, d, 0, main, tail)
            main, tail = score_terms(t, kept)
            main = main + bo[0:64, :]
            tail = tail + bo[64:72, :]
            sc[r, t, 0:64, :] = main
            sc[r, t, 64:72, :] = tail
            seen_main, seen_tail = parts(row_of(ob, t, r))
            tails[2 + t] = pack_score(t, d, 1, main - seen_main, tail - seen_tail)
        sp[d, 256:288, :] = jnp.concatenate(tails, axis=0).astype(BF16)

        @pl.when(has_down if d == 0 else has_up)
        def _():
            x2_copy(d).start()

    def finish_row(t, r, main, tail):
        seen_main, seen_tail = parts(row_of(ob, t, r))
        stack_into(rs.at[r + 1, t], (main - seen_main).astype(BF16), tail - seen_tail, left, right)

    for t in range(OWN):
        for r in (1, 2):
            main, tail = score_terms(t, tuple((i, r + i - 1) for i in range(3)))
            main = main + bo[0:64, :]
            tail = tail + bo[64:72, :]
            put_row(so, t, r, main, tail)
            finish_row(t, r, main, tail)

    for d, r, halo, present in ((0, 0, 0, has_up), (1, 3, 5, has_down)):
        @pl.when(present)
        def _():
            x2_copy(d).wait_recv()
            tails = rp[d, 256:288, :].astype(F32)
            for t in range(OWN):
                sc[r, t, 0:64, :] += rp[d, 64 * t : 64 * t + 64, :].astype(F32)
                sc[r, t, 64:72, :] += tails[8 * t : 8 * t + 8]
                q = 2 + t
                main = kc[1 - d, t, 0:64, :] + rp[d, 64 * q : 64 * q + 64, :].astype(F32)
                tail = kc[1 - d, t, 64:72, :] + tails[8 * q : 8 * q + 8]
                stack_into(rs.at[halo, t], main.astype(BF16), tail, left, right)

    for t in range(OWN):
        for r in (0, 3):
            finish_row(t, r, sc[r, t, 0:64, :], sc[r, t, 64:72, :])

    def grad_hidden(t, r):
        total = None
        for i in range(3):
            term = dot(w2t[i], rs[r + 2 - i, t])
            total = term if total is None else total + term
        gp[r + 1, t] = (total * slope[r, t]).astype(BF16)

    def hidden_outer(n, carry):
        grad_hidden(lax.rem(n, OWN), 3 * (n // OWN))
        return carry

    def hidden_inner(n, carry):
        grad_hidden(lax.rem(n, OWN), 1 + n // OWN)
        return carry

    lax.fori_loop(0, 2 * OWN, hidden_outer, 0, unroll=True)

    @pl.when(has_down)
    def _():
        x3_copy(0).start()

    @pl.when(has_up)
    def _():
        x3_copy(1).start()

    for t in range(OWN):
        for r in (0, 3):
            put_row(so, t, r, sc[r, t, 0:64, :], sc[r, t, 64:72, :])

    lax.fori_loop(0, 2 * OWN, hidden_inner, 0, unroll=True)

    def grad_state(e, r):
        z = None
        for t in range(OWN):
            k = e - t
            if 0 <= k < WINDOW:
                for i in range(3):
                    term = dot(w4[i, k, 0:ZROWS, :], gp[r + 2 - i, t])
                    z = term if z is None else z + term
        return combine(z, left, right)

    def send_row(r):
        for d, e in ((1, 0), (0, 4)):
            main_a, tail_a = grad_state(e, r)
            main_b, tail_b = grad_state(e + 1, r)
            sg[d, r, 0:64, :] = main_a.astype(BF16)
            sg[d, r, 64:80, :] = jnp.concatenate([tail_a, tail_b], axis=0).astype(BF16)
            sg[d, r, 80:144, :] = main_b.astype(BF16)
            g_copy(d, r).start()

    def own_row(r):
        for s in range(OWN):
            main, tail = grad_state(OWN + s, r)
            own[r, s, 0:64, :] = main
            own[r, s, 64:72, :] = tail

    def send_inner(n, carry):
        send_row(1 + n)
        return carry

    def own_inner(n, carry):
        own_row(1 + n)
        return carry

    def send_outer(n, carry):
        send_row(3 * n)
        return carry

    def own_outer(n, carry):
        own_row(3 * n)
        return carry

    lax.fori_loop(0, 2, send_inner, 0, unroll=True)
    lax.fori_loop(0, 2, own_inner, 0, unroll=True)

    @pl.when(has_up)
    def _():
        x3_copy(0).wait_recv()

    @pl.when(has_down)
    def _():
        x3_copy(1).wait_recv()

    lax.fori_loop(0, 2, send_outer, 0, unroll=True)
    lax.fori_loop(0, 2, own_outer, 0, unroll=True)

    for r in (1, 2, 0, 3):
        g_copy(0, r).wait_recv()
        g_copy(1, r).wait_recv()
        tails = rg[0, r, 64:80, :].astype(F32) + rg[1, r, 64:80, :].astype(F32)
        for s in range(OWN):
            low = 80 * s
            main = own[r, s, 0:64, :] + rg[0, r, low : low + 64, :].astype(F32) + rg[1, r, low : low + 64, :].astype(F32)
            tail = own[r, s, 64:72, :] + tails[8 * s : 8 * s + 8]
            put_row(go, s, r, main, tail)

    for d in range(2):
        for s in range(OWN):
            for g in range(2):
                tm_copy(d, s, g).wait_send()
        for r in range(ROWS):
            g_copy(d, r).wait_send()

        @pl.when(has_down if d == 0 else has_up)
        def _():
            for e in range(SPAN):
                lat_copy(d, e, chunk_of(e, 0)).wait_send()
            x2_copy(d).wait_send()
            x3_copy(d).wait_send()


def write_out(so, go, scores_out, guidance_out, sems):
    copies = []
    for s in range(OWN):
        copies.append(pltpu.make_async_copy(so.at[s], scores_out.at[s], sems.at[0, s]))
        copies.append(pltpu.make_async_copy(go.at[s], guidance_out.at[s], sems.at[1, s]))
    for copy in copies:
        copy.start()
    for copy in copies:
        copy.wait()


def solution(mesh):
    whole = P("tm", None, "lat", None)

    def step(states, observed, conv_in, bias_in, conv_out, bias_out):
        shape = states.shape
        dma = pltpu.SemaphoreType.DMA
        hbm = pl.BlockSpec(memory_space=pltpu.HBM)
        vmem = pl.BlockSpec(memory_space=pltpu.VMEM)
        view = (shape[0], shape[1] * shape[2] * 2, 128)

        def seen(x):
            halves = x.reshape(shape[0], shape[1], shape[2], 2, 128)
            return jnp.transpose(halves, (0, 1, 3, 2, 4)).reshape(view)

        def unseen(x):
            halves = x.reshape(shape[0], shape[1], 2, shape[2], 128)
            return jnp.transpose(halves, (0, 1, 3, 2, 4)).reshape(shape)

        so, go = pl.pallas_call(
            kernel,
            out_shape=(pltpu.VMEM(view, F32), pltpu.VMEM(view, F32)),
            in_specs=[hbm, hbm, hbm, vmem, hbm, vmem],
            out_specs=(vmem, vmem),
            scratch_shapes=[
                pltpu.VMEM(view, F32),
                pltpu.VMEM(view, F32),
                pltpu.VMEM((3, 3, WINDOW * C, HID), BF16),
                pltpu.VMEM((3, 3, C, HID), BF16),
                pltpu.VMEM((3, WINDOW, 256, HID), BF16),
                pltpu.VMEM((3, WINDOW, HID, 256), BF16),
                pltpu.VMEM((3, 256, HID), BF16),
                pltpu.VMEM((3, HID, 256), BF16),
                pltpu.VMEM((HID, LON), F32),
                pltpu.VMEM((MAIN + TAIL, LON), F32),
                pltpu.VMEM((OWN, 2, CHUNK, LON), BF16),
                pltpu.VMEM((2, OWN, 2, CHUNK, LON), BF16),
                pltpu.VMEM((2, SPAN, EDGE, LON), BF16),
                pltpu.VMEM((ROWS + 2, SPAN, 256, LON), BF16),
                pltpu.VMEM((OWN, ROWS, HID, LON), F32),
                pltpu.VMEM((ROWS, OWN, HID, LON), F32),
                pltpu.VMEM((ROWS, OWN, HID, LON), BF16),
                pltpu.VMEM((2, 4 * (MAIN + TAIL), LON), BF16),
                pltpu.VMEM((2, 4 * (MAIN + TAIL), LON), BF16),
                pltpu.VMEM((2, OWN, MAIN + TAIL, LON), F32),
                pltpu.VMEM((ROWS, OWN, MAIN + TAIL, LON), F32),
                pltpu.VMEM((ROWS + 2, OWN, 256, LON), BF16),
                pltpu.VMEM((ROWS + 2, OWN, HID, LON), BF16),
                pltpu.VMEM((2, ROWS, CHUNK, LON), BF16),
                pltpu.VMEM((2, ROWS, CHUNK, LON), BF16),
                pltpu.VMEM((ROWS, OWN, MAIN + TAIL, LON), F32),
                dma((4,)),
                dma((2, OWN, 2)),
                dma((2, OWN, 2)),
                dma((2, SPAN)),
                dma((2, SPAN)),
                dma((2,)),
                dma((2,)),
                dma((2,)),
                dma((2,)),
                dma((2, ROWS)),
                dma((2, ROWS)),
            ],
            compiler_params=pltpu.CompilerParams(
                collective_id=0, has_side_effects=True, vmem_limit_bytes=60 * 1024 * 1024
            ),
        )(seen(states), seen(observed), jnp.transpose(conv_in, (0, 1, 3, 2)), bias_in, conv_out, bias_out)
        so, go = (pltpu.with_memory_space_constraint(x, pltpu.VMEM) for x in (so, go))
        scores, guidance = pl.pallas_call(
            write_out,
            out_shape=(jax.ShapeDtypeStruct(view, F32), jax.ShapeDtypeStruct(view, F32)),
            in_specs=[vmem, vmem],
            out_specs=(hbm, hbm),
            scratch_shapes=[dma((2, OWN))],
            compiler_params=pltpu.CompilerParams(vmem_limit_bytes=4 * 1024 * 1024),
        )(so, go)
        return unseen(scores), unseen(guidance)

    sharded = jax.shard_map(
        step, mesh=mesh, in_specs=(whole, whole, P(), P(), P(), P()), out_specs=(whole, whole), check_vma=False
    )

    def run(*args):
        with jax.sharding.use_abstract_mesh(mesh.abstract_mesh):
            return sharded(*args)

    return run
```

```python
import jax
import jax.numpy as jnp
from jax import lax
from jax.experimental import pallas as pl
from jax.experimental.pallas import tpu as pltpu
from jax.sharding import PartitionSpec as P

MESH = pl.DeviceIdType.MESH
F32 = jnp.float32
BF16 = jnp.bfloat16
C = 69
HID = 256
WINDOW = 5
LON = 256
ROWS = 4
OWN = 2
SPAN = OWN + WINDOW - 1
MAIN = 64
TAIL = 8
STACK = 3 * (MAIN + TAIL)
ZROWS = 224
CHUNK = 2 * MAIN + 2 * TAIL
EDGE = MAIN + 2 * TAIL


def dot(a, b):
    return jnp.dot(a, b, preferred_element_type=F32)


def parts(x):
    tail = jnp.concatenate([x[MAIN:], jnp.zeros((MAIN + TAIL - C, x.shape[1]), F32)], axis=0)
    return x[:MAIN], tail


def row_of(ref, s, r):
    return jnp.concatenate([ref[s, pl.ds(ROWS * h + r, C, stride=2 * ROWS), :] for h in range(2)], axis=1)


def put_row(ref, s, r, main, tail):
    for h in range(2):
        lanes = slice(128 * h, 128 * h + 128)
        ref[s, pl.ds(ROWS * h + r, MAIN, stride=2 * ROWS), :] = main[:, lanes]
        ref[s, pl.ds(2 * ROWS * MAIN + ROWS * h + r, C - MAIN, stride=2 * ROWS), :] = tail[: C - MAIN, lanes]


def left(x):
    return pltpu.roll(x, LON - 1, axis=1)


def right(x):
    return pltpu.roll(x, 1, axis=1)


def stack_into(ref, main, tail, first, last):
    ref[0:64, :] = first(main)
    ref[64:128, :] = main
    ref[128:192, :] = last(main)
    tails = jnp.concatenate([first(tail), tail, last(tail), jnp.zeros((TAIL, LON), F32)], axis=0)
    ref[192:224, :] = tails.astype(BF16)


def combine(z, first, last):
    main = first(z[0:64]) + z[64:128] + last(z[128:192])
    tail = first(z[192:200]) + z[200:208] + last(z[208:216])
    return main, tail


def kernel(
    states, observed, conv_in, bias_in, conv_out, bias_out, so, go,
    st, ob, wi, wo, w4, w1, w2, w2t, bi, bo, sbuf, rbuf, hb, xs, pre, slope, act, sp, rp, kc, sc,
    rs, gp, sg, rg, own, near, b1, b2,
    local, tm_send, tm_recv, lat_send, lat_recv, x2_send, x2_recv, x3_send, x3_recv, g_send, g_recv,
):
    m = lax.axis_index("tm")
    l = lax.axis_index("lat")
    count_m = lax.axis_size("tm")
    count_l = lax.axis_size("lat")
    nxt = lax.rem(m + 1, count_m)
    prv = lax.rem(m + count_m - 1, count_m)
    has_up = l > 0
    has_down = l < count_l - 1

    load_st = pltpu.make_async_copy(states, st, local.at[0])
    load_wi = pltpu.make_async_copy(conv_in, wi, local.at[1])
    load_wo = pltpu.make_async_copy(conv_out, wo, local.at[2])
    load_ob = pltpu.make_async_copy(observed, ob, local.at[3])
    load_st.start()
    load_wi.start()
    load_wo.start()
    load_ob.start()
    load_b1 = pltpu.make_async_copy(bias_in, b1, local.at[4])
    load_b2 = pltpu.make_async_copy(bias_out, b2, local.at[5])
    load_b1.start()
    load_b2.start()

    barrier = pltpu.get_barrier_semaphore()
    pl.semaphore_signal(barrier, inc=1, device_id=(nxt, l), device_id_type=MESH)
    pl.semaphore_signal(barrier, inc=1, device_id=(prv, l), device_id_type=MESH)

    @pl.when(has_up)
    def _():
        pl.semaphore_signal(barrier, inc=1, device_id=(m, l - 1), device_id_type=MESH)

    @pl.when(has_down)
    def _():
        pl.semaphore_signal(barrier, inc=1, device_id=(m, l + 1), device_id_type=MESH)

    def remote(src, dst, send, recv, where):
        return pltpu.make_async_remote_copy(
            src_ref=src, dst_ref=dst, send_sem=send, recv_sem=recv, device_id=where, device_id_type=MESH
        )

    def tm_copy(d, s, g):
        where = (nxt, l) if d == 0 else (prv, l)
        return remote(sbuf.at[s, g], rbuf.at[d, s, g], tm_send.at[d, s, g], tm_recv.at[d, s, g], where)

    def lat_copy(d, e, chunk):
        if d == 0:
            return remote(chunk.at[pl.ds(MAIN, EDGE)], hb.at[0, e], lat_send.at[0, e], lat_recv.at[0, e], (m, l + 1))
        return remote(chunk.at[pl.ds(0, EDGE)], hb.at[1, e], lat_send.at[1, e], lat_recv.at[1, e], (m, l - 1))

    def chunk_of(e, g):
        if e < OWN:
            return rbuf.at[0, e, g]
        if e < 2 * OWN:
            return sbuf.at[e - OWN, g]
        return rbuf.at[1, e - 2 * OWN, g]

    def lat_start(e):
        @pl.when(has_down)
        def _():
            lat_copy(0, e, chunk_of(e, 0)).start()

        @pl.when(has_up)
        def _():
            lat_copy(1, e, chunk_of(e, 0)).start()

    def x2_copy(d):
        where = (m, l + 1) if d == 0 else (m, l - 1)
        return remote(sp.at[d], rp.at[d], x2_send.at[d], x2_recv.at[d], where)

    def x3_copy(d):
        if d == 0:
            return remote(gp.at[4], gp.at[0], x3_send.at[0], x3_recv.at[0], (m, l + 1))
        return remote(gp.at[1], gp.at[5], x3_send.at[1], x3_recv.at[1], (m, l - 1))

    def g_copy(d, r):
        where = (nxt, l) if d == 0 else (prv, l)
        return remote(sg.at[d, r], rg.at[d, r], g_send.at[d, r], g_recv.at[d, r], where)

    load_st.wait()
    for g, (a, b) in enumerate(((0, 3), (1, 2))):
        for s in range(OWN):
            main_a, tail_a = parts(row_of(st, s, a))
            main_b, tail_b = parts(row_of(st, s, b))
            sbuf[s, g, 0:64, :] = main_a.astype(BF16)
            sbuf[s, g, 64:80, :] = jnp.concatenate([tail_a, tail_b], axis=0).astype(BF16)
            sbuf[s, g, 80:144, :] = main_b.astype(BF16)
        if g == 0:
            pl.semaphore_wait(barrier, 2 + has_up.astype(jnp.int32) + has_down.astype(jnp.int32))

        tm_copy(0, 1, g).start()
        tm_copy(1, 0, g).start()
        tm_copy(0, 0, g).start()
        tm_copy(1, 1, g).start()
        if g == 0:
            for s in range(OWN):
                lat_start(OWN + s)

    def zero_pads(n, carry):
        xs[n // SPAN, lax.rem(n, SPAN), ZROWS:256, :] = jnp.zeros((256 - ZROWS, LON), BF16)
        return carry

    lax.fori_loop(0, (ROWS + 2) * SPAN, zero_pads, 0)
    for rho in range(ROWS + 2):
        for t in range(OWN):
            rs[rho, t, ZROWS:256, :] = jnp.zeros((256 - ZROWS, LON), BF16)

    def zero_halo(rho):
        def one(e, carry):
            xs[rho, e, 0:ZROWS, :] = jnp.zeros((ZROWS, LON), BF16)
            return carry

        lax.fori_loop(0, SPAN, one, 0)
        for t in range(OWN):
            rs[rho, t, 0:ZROWS, :] = jnp.zeros((ZROWS, LON), BF16)
            gp[rho, t] = jnp.zeros((HID, LON), BF16)

    @pl.when(jnp.logical_not(has_up))
    def _():
        zero_halo(0)

    @pl.when(jnp.logical_not(has_down))
    def _():
        zero_halo(ROWS + 1)

    load_b1.wait()
    load_b2.wait()
    bi[...] = jnp.broadcast_to(b1[...][None, :], (HID, HID)).T
    row = jnp.concatenate([b2[...][None, :], jnp.zeros((1, 128 - C), F32)], axis=1)
    column = jnp.broadcast_to(row, (128, 128)).T
    bo[...] = jnp.concatenate([column[: MAIN + TAIL], column[: MAIN + TAIL]], axis=1)

    load_wi.wait()

    def weights(i, carry):
        for k in range(WINDOW):
            tails = []
            for j in range(3):
                low = (C * k) // 16 * 16
                high = min((C * k + C + 15) // 16 * 16, WINDOW * C)
                piece = wi[i, j, low:high, :].astype(F32)[C * k - low : C * k - low + C]
                main, tail = parts(piece)
                w4[i, k, 64 * j : 64 * j + 64, :] = main.astype(BF16)
                tails.append(tail)
            tails.append(jnp.zeros((MAIN - 3 * TAIL, HID), F32))
            w4[i, k, 192:256, :] = jnp.concatenate(tails, axis=0).astype(BF16)
            w1[i, k] = w4[i, k].T
        return carry

    lax.fori_loop(0, 3, weights, 0)
    load_wo.wait()
    for i in range(3):
        tails = []
        for j in range(3):
            main, tail = parts(wo[i, j].astype(F32))
            w2[i, 64 * j : 64 * j + 64, :] = main.astype(BF16)
            tails.append(tail)
        tails.append(jnp.zeros((MAIN - 3 * TAIL, HID), F32))
        w2[i, 192:256, :] = jnp.concatenate(tails, axis=0).astype(BF16)
        w2t[i] = w2[i].T

    def stack_chunk(e, g):
        chunk = chunk_of(e, g)
        tails = chunk[64:80, :].astype(F32)
        a, b = ((0, 3), (1, 2))[g]
        stack_into(xs.at[a + 1, e], chunk[0:64, :], tails[0:8], right, left)
        stack_into(xs.at[b + 1, e], chunk[80:144, :], tails[8:16], right, left)

    def stack_halo(e):
        @pl.when(has_up)
        def _():
            lat_copy(0, e, chunk_of(e, 0)).wait_recv()
            stack_into(xs.at[0, e], hb[0, e, 16:80, :], hb[0, e, 0:16, :].astype(F32)[8:16], right, left)

        @pl.when(has_down)
        def _():
            lat_copy(1, e, chunk_of(e, 0)).wait_recv()
            stack_into(xs.at[5, e], hb[1, e, 0:64, :], hb[1, e, 64:80, :].astype(F32)[0:8], right, left)

    for s in range(OWN):
        stack_chunk(OWN + s, 0)
        stack_chunk(OWN + s, 1)

    def conv_states(t, r, total, picks):
        for e in picks:
            for i in range(3):
                total = total + dot(w1[i, e - t], xs[r + i, e])
        return total

    def phase_own(n, carry):
        t = lax.rem(n, OWN)
        r = n // OWN
        pre[t, r] = conv_states(t, r, bi[...], (2, 3))
        return carry

    for s in range(OWN):
        stack_halo(OWN + s)
    tm_copy(0, 1, 0).wait_recv()
    lat_start(1)
    tm_copy(1, 0, 0).wait_recv()
    lat_start(4)
    lax.fori_loop(0, OWN * ROWS // 2, phase_own, 0, unroll=True)
    tm_copy(0, 0, 0).wait_recv()
    lat_start(0)
    tm_copy(1, 1, 0).wait_recv()
    lat_start(5)
    stack_chunk(1, 0)
    stack_chunk(4, 0)
    lax.fori_loop(OWN * ROWS // 2, OWN * ROWS, phase_own, 0, unroll=True)
    stack_chunk(0, 0)
    stack_chunk(5, 0)
    tm_copy(0, 1, 1).wait_recv()
    tm_copy(1, 0, 1).wait_recv()
    stack_chunk(1, 1)
    stack_chunk(4, 1)
    stack_halo(1)
    stack_halo(4)

    def phase_near(n, carry):
        t = lax.rem(n, OWN)
        r = n // OWN
        pre[t, r] = conv_states(t, r, pre[t, r], (1, 4))
        return carry

    lax.fori_loop(0, OWN * ROWS, phase_near, 0, unroll=True)
    tm_copy(0, 0, 1).wait_recv()
    tm_copy(1, 1, 1).wait_recv()
    stack_chunk(0, 1)
    stack_chunk(5, 1)
    stack_halo(0)
    stack_halo(5)

    def phase_far(n, carry):
        t = lax.rem(n, OWN)
        r = n // OWN
        v = pre[t, r]
        for i in range(3):
            v = v + dot(w1[i, 4 * t], xs[r + i, 5 * t])
        sig = 0.5 + 0.5 * jnp.tanh(0.5 * v)
        act[r, t] = (v * sig).astype(BF16)
        slope[r, t] = sig * (1.0 + v * (1.0 - sig))
        return carry

    lax.fori_loop(0, OWN * ROWS, phase_far, 0, unroll=True)

    load_ob.wait()

    def score_terms(t, pairs):
        z = None
        for i, r in pairs:
            term = dot(w2[i, 0:ZROWS, :], act[r, t])
            z = term if z is None else z + term
        return combine(z, right, left)

    def pack_score(t, d, kind, main, tail):
        q = 2 * kind + t
        sp[d, 64 * q : 64 * q + 64, :] = main.astype(BF16)
        return tail

    for d, given, kept, r in ((0, ((0, 3),), ((0, 2), (1, 3)), 3), (1, ((2, 0),), ((1, 0), (2, 1)), 0)):
        tails = [None] * 4
        for t in range(OWN):
            main, tail = score_terms(t, given)
            kc[d, t, 0:64, :] = main
            kc[d, t, 64:72, :] = tail
            tails[t] = pack_score(t, d, 0, main, tail)
            main, tail = score_terms(t, kept)
            main = main + bo[0:64, :]
            tail = tail + bo[64:72, :]
            sc[r, t, 0:64, :] = main
            sc[r, t, 64:72, :] = tail
            seen_main, seen_tail = parts(row_of(ob, t, r))
            tails[2 + t] = pack_score(t, d, 1, main - seen_main, tail - seen_tail)
        sp[d, 256:288, :] = jnp.concatenate(tails, axis=0).astype(BF16)

        @pl.when(has_down if d == 0 else has_up)
        def _():
            x2_copy(d).start()

    def finish_row(t, r, main, tail):
        seen_main, seen_tail = parts(row_of(ob, t, r))
        stack_into(rs.at[r + 1, t], (main - seen_main).astype(BF16), tail - seen_tail, left, right)

    for t in range(OWN):
        for r in (1, 2):
            main, tail = score_terms(t, tuple((i, r + i - 1) for i in range(3)))
            main = main + bo[0:64, :]
            tail = tail + bo[64:72, :]
            put_row(so, t, r, main, tail)
            finish_row(t, r, main, tail)

    for d, r, halo, present in ((0, 0, 0, has_up), (1, 3, 5, has_down)):
        @pl.when(present)
        def _():
            x2_copy(d).wait_recv()
            tails = rp[d, 256:288, :].astype(F32)
            for t in range(OWN):
                sc[r, t, 0:64, :] += rp[d, 64 * t : 64 * t + 64, :].astype(F32)
                sc[r, t, 64:72, :] += tails[8 * t : 8 * t + 8]
                q = 2 + t
                main = kc[1 - d, t, 0:64, :] + rp[d, 64 * q : 64 * q + 64, :].astype(F32)
                tail = kc[1 - d, t, 64:72, :] + tails[8 * q : 8 * q + 8]
                stack_into(rs.at[halo, t], main.astype(BF16), tail, left, right)

    for t in range(OWN):
        for r in (0, 3):
            finish_row(t, r, sc[r, t, 0:64, :], sc[r, t, 64:72, :])

    def grad_hidden(t, r):
        total = None
        for i in range(3):
            term = dot(w2t[i], rs[r + 2 - i, t])
            total = term if total is None else total + term
        gp[r + 1, t] = (total * slope[r, t]).astype(BF16)

    def hidden_outer(n, carry):
        grad_hidden(lax.rem(n, OWN), 3 * (n // OWN))
        return carry

    def hidden_inner(n, carry):
        grad_hidden(lax.rem(n, OWN), 1 + n // OWN)
        return carry

    lax.fori_loop(0, 2 * OWN, hidden_outer, 0, unroll=True)

    @pl.when(has_down)
    def _():
        x3_copy(0).start()

    @pl.when(has_up)
    def _():
        x3_copy(1).start()

    for t in range(OWN):
        for r in (0, 3):
            put_row(so, t, r, sc[r, t, 0:64, :], sc[r, t, 64:72, :])

    lax.fori_loop(0, 2 * OWN, hidden_inner, 0, unroll=True)

    def grad_state(e, r, taps=(0, 1, 2)):
        z = None
        for t in range(OWN):
            k = e - t
            if 0 <= k < WINDOW:
                for i in taps:
                    term = dot(w4[i, k, 0:ZROWS, :], gp[r + 2 - i, t])
                    z = term if z is None else z + term
        return combine(z, left, right)

    sides = ((1, 0), (0, 4))

    def pack_row(d, r, pair):
        (main_a, tail_a), (main_b, tail_b) = pair
        sg[d, r, 0:64, :] = main_a.astype(BF16)
        sg[d, r, 64:80, :] = jnp.concatenate([tail_a, tail_b], axis=0).astype(BF16)
        sg[d, r, 80:144, :] = main_b.astype(BF16)

    def own_rows(rows):
        for r in rows:
            for s in range(OWN):
                main, tail = grad_state(OWN + s, r)
                own[r, s, 0:64, :] = main
                own[r, s, 64:72, :] = tail

    for r in (1, 2):
        for d, e in sides:
            pack_row(d, r, [grad_state(e + s, r) for s in range(OWN)])
    for r in (1, 2):
        for d, e in sides:
            g_copy(d, r).start()

    for n, (r, taps) in enumerate(((0, (0, 1)), (3, (1, 2)))):
        for d, e in sides:
            for s in range(OWN):
                main, tail = grad_state(e + s, r, taps)
                near[n, d, s, 0:64, :] = main
                near[n, d, s, 64:72, :] = tail
    own_rows((1, 2))

    for n, (r, tap, present) in enumerate(((0, 2, has_up), (3, 0, has_down))):
        @pl.when(present)
        def _():
            x3_copy(n).wait_recv()

        for d, e in sides:
            pair = []
            for s in range(OWN):
                main, tail = grad_state(e + s, r, (tap,))
                pair.append((main + near[n, d, s, 0:64, :], tail + near[n, d, s, 64:72, :]))
            pack_row(d, r, pair)
        for d, e in sides:
            g_copy(d, r).start()

    own_rows((0, 3))

    for d in range(2):
        for s in range(OWN):
            for g in range(2):
                tm_copy(d, s, g).wait_send()

        @pl.when(has_down if d == 0 else has_up)
        def _():
            for e in range(SPAN):
                lat_copy(d, e, chunk_of(e, 0)).wait_send()
            x2_copy(d).wait_send()
            x3_copy(d).wait_send()

    for r in (1, 2, 0, 3):
        g_copy(0, r).wait_recv()
        g_copy(1, r).wait_recv()
        tails = rg[0, r, 64:80, :].astype(F32) + rg[1, r, 64:80, :].astype(F32)
        for s in range(OWN):
            low = 80 * s
            main = own[r, s, 0:64, :] + rg[0, r, low : low + 64, :].astype(F32) + rg[1, r, low : low + 64, :].astype(F32)
            tail = own[r, s, 64:72, :] + tails[8 * s : 8 * s + 8]
            put_row(go, s, r, main, tail)

    for d in range(2):
        for r in range(ROWS):
            g_copy(d, r).wait_send()


def write_out(so, go, scores_out, guidance_out, sems):
    copies = []
    for s in range(OWN):
        copies.append(pltpu.make_async_copy(so.at[s], scores_out.at[s], sems.at[0, s]))
        copies.append(pltpu.make_async_copy(go.at[s], guidance_out.at[s], sems.at[1, s]))
    for copy in copies:
        copy.start()
    for copy in copies:
        copy.wait()


def solution(mesh):
    whole = P("tm", None, "lat", None)

    def step(states, observed, conv_in, bias_in, conv_out, bias_out):
        shape = states.shape
        dma = pltpu.SemaphoreType.DMA
        hbm = pl.BlockSpec(memory_space=pltpu.HBM)
        vmem = pl.BlockSpec(memory_space=pltpu.VMEM)
        view = (shape[0], shape[1] * shape[2] * 2, 128)

        def seen(x):
            halves = x.reshape(shape[0], shape[1], shape[2], 2, 128)
            return jnp.transpose(halves, (0, 1, 3, 2, 4)).reshape(view)

        def unseen(x):
            halves = x.reshape(shape[0], shape[1], 2, shape[2], 128)
            return jnp.transpose(halves, (0, 1, 3, 2, 4)).reshape(shape)

        so, go = pl.pallas_call(
            kernel,
            out_shape=(pltpu.VMEM(view, F32), pltpu.VMEM(view, F32)),
            in_specs=[hbm] * 6,
            out_specs=(vmem, vmem),
            scratch_shapes=[
                pltpu.VMEM(view, F32),
                pltpu.VMEM(view, F32),
                pltpu.VMEM((3, 3, WINDOW * C, HID), BF16),
                pltpu.VMEM((3, 3, C, HID), BF16),
                pltpu.VMEM((3, WINDOW, 256, HID), BF16),
                pltpu.VMEM((3, WINDOW, HID, 256), BF16),
                pltpu.VMEM((3, 256, HID), BF16),
                pltpu.VMEM((3, HID, 256), BF16),
                pltpu.VMEM((HID, LON), F32),
                pltpu.VMEM((MAIN + TAIL, LON), F32),
                pltpu.VMEM((OWN, 2, CHUNK, LON), BF16),
                pltpu.VMEM((2, OWN, 2, CHUNK, LON), BF16),
                pltpu.VMEM((2, SPAN, EDGE, LON), BF16),
                pltpu.VMEM((ROWS + 2, SPAN, 256, LON), BF16),
                pltpu.VMEM((OWN, ROWS, HID, LON), F32),
                pltpu.VMEM((ROWS, OWN, HID, LON), F32),
                pltpu.VMEM((ROWS, OWN, HID, LON), BF16),
                pltpu.VMEM((2, 4 * (MAIN + TAIL), LON), BF16),
                pltpu.VMEM((2, 4 * (MAIN + TAIL), LON), BF16),
                pltpu.VMEM((2, OWN, MAIN + TAIL, LON), F32),
                pltpu.VMEM((ROWS, OWN, MAIN + TAIL, LON), F32),
                pltpu.VMEM((ROWS + 2, OWN, 256, LON), BF16),
                pltpu.VMEM((ROWS + 2, OWN, HID, LON), BF16),
                pltpu.VMEM((2, ROWS, CHUNK, LON), BF16),
                pltpu.VMEM((2, ROWS, CHUNK, LON), BF16),
                pltpu.VMEM((ROWS, OWN, MAIN + TAIL, LON), F32),
                pltpu.VMEM((2, 2, OWN, MAIN + TAIL, LON), F32),
                pltpu.VMEM((HID,), F32),
                pltpu.VMEM((C,), F32),
                dma((6,)),
                dma((2, OWN, 2)),
                dma((2, OWN, 2)),
                dma((2, SPAN)),
                dma((2, SPAN)),
                dma((2,)),
                dma((2,)),
                dma((2,)),
                dma((2,)),
                dma((2, ROWS)),
                dma((2, ROWS)),
            ],
            compiler_params=pltpu.CompilerParams(
                collective_id=0, has_side_effects=True, vmem_limit_bytes=60 * 1024 * 1024
            ),
        )(seen(states), seen(observed), jnp.transpose(conv_in, (0, 1, 3, 2)), bias_in, conv_out, bias_out)
        so, go = (pltpu.with_memory_space_constraint(x, pltpu.VMEM) for x in (so, go))
        scores, guidance = pl.pallas_call(
            write_out,
            out_shape=(jax.ShapeDtypeStruct(view, F32), jax.ShapeDtypeStruct(view, F32)),
            in_specs=[vmem, vmem],
            out_specs=(hbm, hbm),
            scratch_shapes=[dma((2, OWN))],
            compiler_params=pltpu.CompilerParams(vmem_limit_bytes=4 * 1024 * 1024),
        )(so, go)
        return unseen(scores), unseen(guidance)

    sharded = jax.shard_map(
        step, mesh=mesh, in_specs=(whole, whole, P(), P(), P(), P()), out_specs=(whole, whole), check_vma=False
    )

    def run(*args):
        with jax.sharding.use_abstract_mesh(mesh.abstract_mesh):
            return sharded(*args)

    return run
```

```python
import jax
import jax.numpy as jnp
from jax import lax
from jax.experimental import pallas as pl
from jax.experimental.pallas import tpu as pltpu
from jax.sharding import PartitionSpec as P

MESH = pl.DeviceIdType.MESH
F32 = jnp.float32
BF16 = jnp.bfloat16
C = 69
HID = 256
WINDOW = 5
LON = 256
ROWS = 4
OWN = 2
SPAN = OWN + WINDOW - 1
MAIN = 64
TAIL = 8
STACK = 3 * (MAIN + TAIL)
ZROWS = 224
CHUNK = 2 * MAIN + 2 * TAIL
EDGE = MAIN + 2 * TAIL


def dot(a, b):
    return jnp.dot(a, b, preferred_element_type=F32)


def parts(x):
    tail = jnp.concatenate([x[MAIN:], jnp.zeros((MAIN + TAIL - C, x.shape[1]), F32)], axis=0)
    return x[:MAIN], tail


def row_of(ref, s, r):
    return jnp.concatenate([ref[s, pl.ds(ROWS * h + r, C, stride=2 * ROWS), :] for h in range(2)], axis=1)


def put_row(ref, s, r, main, tail):
    for h in range(2):
        lanes = slice(128 * h, 128 * h + 128)
        ref[s, pl.ds(ROWS * h + r, MAIN, stride=2 * ROWS), :] = main[:, lanes]
        ref[s, pl.ds(2 * ROWS * MAIN + ROWS * h + r, C - MAIN, stride=2 * ROWS), :] = tail[: C - MAIN, lanes]


def left(x):
    return pltpu.roll(x, LON - 1, axis=1)


def right(x):
    return pltpu.roll(x, 1, axis=1)


def stack_into(ref, main, tail, first, last):
    ref[0:64, :] = first(main)
    ref[64:128, :] = main
    ref[128:192, :] = last(main)
    tails = jnp.concatenate([first(tail), tail, last(tail), jnp.zeros((TAIL, LON), F32)], axis=0)
    ref[192:224, :] = tails.astype(BF16)


def combine(z, first, last):
    main = first(z[0:64]) + z[64:128] + last(z[128:192])
    tail = first(z[192:200]) + z[200:208] + last(z[208:216])
    return main, tail


def kernel(
    states, observed, conv_in, bias_in, conv_out, bias_out, so, go,
    st, ob, wi, wo, w4, w1, w2, w2t, bi, bo, sbuf, rbuf, hb, xs, pre, slope, act, sp, rp, kc, sc,
    rs, gp, sg, rg, own, near, b1, b2,
    local, tm_send, tm_recv, lat_send, lat_recv, x2_send, x2_recv, x3_send, x3_recv, g_send, g_recv,
):
    m = lax.axis_index("tm")
    l = lax.axis_index("lat")
    count_m = lax.axis_size("tm")
    count_l = lax.axis_size("lat")
    nxt = lax.rem(m + 1, count_m)
    prv = lax.rem(m + count_m - 1, count_m)
    has_up = l > 0
    has_down = l < count_l - 1

    load_st = pltpu.make_async_copy(states, st, local.at[0])
    load_wi = pltpu.make_async_copy(conv_in, wi, local.at[1])
    load_wo = pltpu.make_async_copy(conv_out, wo, local.at[2])
    load_ob = pltpu.make_async_copy(observed, ob, local.at[3])
    load_st.start()
    load_wi.start()
    load_wo.start()
    load_ob.start()
    load_b1 = pltpu.make_async_copy(bias_in, b1, local.at[4])
    load_b2 = pltpu.make_async_copy(bias_out, b2, local.at[5])
    load_b1.start()
    load_b2.start()

    barrier = pltpu.get_barrier_semaphore()
    pl.semaphore_signal(barrier, inc=1, device_id=(nxt, l), device_id_type=MESH)
    pl.semaphore_signal(barrier, inc=1, device_id=(prv, l), device_id_type=MESH)

    @pl.when(has_up)
    def _():
        pl.semaphore_signal(barrier, inc=1, device_id=(m, l - 1), device_id_type=MESH)

    @pl.when(has_down)
    def _():
        pl.semaphore_signal(barrier, inc=1, device_id=(m, l + 1), device_id_type=MESH)

    def remote(src, dst, send, recv, where):
        return pltpu.make_async_remote_copy(
            src_ref=src, dst_ref=dst, send_sem=send, recv_sem=recv, device_id=where, device_id_type=MESH
        )

    def tm_copy(d, s, g):
        where = (nxt, l) if d == 0 else (prv, l)
        return remote(sbuf.at[s, g], rbuf.at[d, s, g], tm_send.at[d], tm_recv.at[d, s, g], where)

    def lat_copy(d, e, chunk):
        if d == 0:
            return remote(chunk.at[pl.ds(MAIN, EDGE)], hb.at[0, e], lat_send.at[0], lat_recv.at[0, e], (m, l + 1))
        return remote(chunk.at[pl.ds(0, EDGE)], hb.at[1, e], lat_send.at[1], lat_recv.at[1, e], (m, l - 1))

    def chunk_of(e, g):
        if e < OWN:
            return rbuf.at[0, e, g]
        if e < 2 * OWN:
            return sbuf.at[e - OWN, g]
        return rbuf.at[1, e - 2 * OWN, g]

    def lat_start(e):
        @pl.when(has_down)
        def _():
            lat_copy(0, e, chunk_of(e, 0)).start()

        @pl.when(has_up)
        def _():
            lat_copy(1, e, chunk_of(e, 0)).start()

    def x2_copy(d, t):
        where = (m, l + 1) if d == 0 else (m, l - 1)
        return remote(sp.at[d, t], rp.at[d, t], x2_send.at[d, t], x2_recv.at[d, t], where)

    def x3_copy(d):
        if d == 0:
            return remote(gp.at[4], gp.at[0], x3_send.at[0], x3_recv.at[0], (m, l + 1))
        return remote(gp.at[1], gp.at[5], x3_send.at[1], x3_recv.at[1], (m, l - 1))

    def g_copy(d, r):
        where = (nxt, l) if d == 0 else (prv, l)
        return remote(sg.at[d, r], rg.at[d, r], g_send.at[d], g_recv.at[d, r], where)

    load_st.wait()
    for g, (a, b) in enumerate(((0, 3), (1, 2))):
        for s in range(OWN):
            main_a, tail_a = parts(row_of(st, s, a))
            main_b, tail_b = parts(row_of(st, s, b))
            sbuf[s, g, 0:64, :] = main_a.astype(BF16)
            sbuf[s, g, 64:80, :] = jnp.concatenate([tail_a, tail_b], axis=0).astype(BF16)
            sbuf[s, g, 80:144, :] = main_b.astype(BF16)
        if g == 0:
            pl.semaphore_wait(barrier, 2 + has_up.astype(jnp.int32) + has_down.astype(jnp.int32))

        tm_copy(0, 1, g).start()
        tm_copy(1, 0, g).start()
        tm_copy(0, 0, g).start()
        tm_copy(1, 1, g).start()
        if g == 0:
            for s in range(OWN):
                lat_start(OWN + s)

    def zero_pads(n, carry):
        xs[n // SPAN, lax.rem(n, SPAN), ZROWS:256, :] = jnp.zeros((256 - ZROWS, LON), BF16)
        return carry

    lax.fori_loop(0, (ROWS + 2) * SPAN, zero_pads, 0)
    for rho in range(ROWS + 2):
        for t in range(OWN):
            rs[rho, t, ZROWS:256, :] = jnp.zeros((256 - ZROWS, LON), BF16)

    def zero_halo(rho):
        def one(e, carry):
            xs[rho, e, 0:ZROWS, :] = jnp.zeros((ZROWS, LON), BF16)
            return carry

        lax.fori_loop(0, SPAN, one, 0)
        for t in range(OWN):
            rs[rho, t, 0:ZROWS, :] = jnp.zeros((ZROWS, LON), BF16)
            gp[rho, t] = jnp.zeros((HID, LON), BF16)

    @pl.when(jnp.logical_not(has_up))
    def _():
        zero_halo(0)

    @pl.when(jnp.logical_not(has_down))
    def _():
        zero_halo(ROWS + 1)

    load_b1.wait()
    load_b2.wait()
    bi[...] = jnp.broadcast_to(b1[...][None, :], (HID, HID)).T
    row = jnp.concatenate([b2[...][None, :], jnp.zeros((1, 128 - C), F32)], axis=1)
    column = jnp.broadcast_to(row, (128, 128)).T
    bo[...] = jnp.concatenate([column[: MAIN + TAIL], column[: MAIN + TAIL]], axis=1)

    load_wi.wait()

    def weights(i, carry):
        for k in range(WINDOW):
            tails = []
            for j in range(3):
                low = (C * k) // 16 * 16
                high = min((C * k + C + 15) // 16 * 16, WINDOW * C)
                piece = wi[i, j, low:high, :].astype(F32)[C * k - low : C * k - low + C]
                main, tail = parts(piece)
                w4[i, k, 64 * j : 64 * j + 64, :] = main.astype(BF16)
                tails.append(tail)
            tails.append(jnp.zeros((MAIN - 3 * TAIL, HID), F32))
            w4[i, k, 192:256, :] = jnp.concatenate(tails, axis=0).astype(BF16)
            w1[i, k] = w4[i, k].T
        return carry

    lax.fori_loop(0, 3, weights, 0)
    load_wo.wait()
    for i in range(3):
        tails = []
        for j in range(3):
            main, tail = parts(wo[i, j].astype(F32))
            w2[i, 64 * j : 64 * j + 64, :] = main.astype(BF16)
            tails.append(tail)
        tails.append(jnp.zeros((MAIN - 3 * TAIL, HID), F32))
        w2[i, 192:256, :] = jnp.concatenate(tails, axis=0).astype(BF16)
        w2t[i] = w2[i].T

    def stack_chunk(e, g):
        chunk = chunk_of(e, g)
        tails = chunk[64:80, :].astype(F32)
        a, b = ((0, 3), (1, 2))[g]
        stack_into(xs.at[a + 1, e], chunk[0:64, :], tails[0:8], right, left)
        stack_into(xs.at[b + 1, e], chunk[80:144, :], tails[8:16], right, left)

    def stack_halo(e):
        @pl.when(has_up)
        def _():
            lat_copy(0, e, chunk_of(e, 0)).wait_recv()
            stack_into(xs.at[0, e], hb[0, e, 16:80, :], hb[0, e, 0:16, :].astype(F32)[8:16], right, left)

        @pl.when(has_down)
        def _():
            lat_copy(1, e, chunk_of(e, 0)).wait_recv()
            stack_into(xs.at[5, e], hb[1, e, 0:64, :], hb[1, e, 64:80, :].astype(F32)[0:8], right, left)

    for s in range(OWN):
        stack_chunk(OWN + s, 0)
        stack_chunk(OWN + s, 1)

    def conv_states(t, r, total, picks):
        for e in picks:
            for i in range(3):
                total = total + dot(w1[i, e - t], xs[r + i, e])
        return total

    def phase_own(n, carry):
        t = lax.rem(n, OWN)
        r = n // OWN
        pre[t, r] = conv_states(t, r, bi[...], (2, 3))
        return carry

    for s in range(OWN):
        stack_halo(OWN + s)
    tm_copy(0, 1, 0).wait_recv()
    lat_start(1)
    tm_copy(1, 0, 0).wait_recv()
    lat_start(4)
    lax.fori_loop(0, OWN * ROWS // 2, phase_own, 0, unroll=True)
    tm_copy(0, 0, 0).wait_recv()
    lat_start(0)
    tm_copy(1, 1, 0).wait_recv()
    lat_start(5)
    stack_chunk(1, 0)
    stack_chunk(4, 0)
    lax.fori_loop(OWN * ROWS // 2, OWN * ROWS, phase_own, 0, unroll=True)
    stack_chunk(0, 0)
    stack_chunk(5, 0)
    tm_copy(0, 1, 1).wait_recv()
    tm_copy(1, 0, 1).wait_recv()
    stack_chunk(1, 1)
    stack_chunk(4, 1)

    inner = ((0, 1), (1, 1), (0, 2), (1, 2))
    outer = ((0, 0), (1, 0), (0, 3), (1, 3))

    def phase_near(t, r):
        pre[t, r] = conv_states(t, r, pre[t, r], (1, 4))

    def phase_far(t, r):
        v = pre[t, r]
        for i in range(3):
            v = v + dot(w1[i, 4 * t], xs[r + i, 5 * t])
        sig = 0.5 + 0.5 * jnp.tanh(0.5 * v)
        act[r, t] = (v * sig).astype(BF16)
        slope[r, t] = sig * (1.0 + v * (1.0 - sig))

    for t, r in inner:
        phase_near(t, r)
    stack_halo(1)
    stack_halo(4)
    for t, r in outer:
        phase_near(t, r)
    tm_copy(0, 0, 1).wait_recv()
    tm_copy(1, 1, 1).wait_recv()
    stack_chunk(0, 1)
    stack_chunk(5, 1)
    for t, r in inner:
        phase_far(t, r)
    stack_halo(0)
    stack_halo(5)
    for t, r in outer:
        phase_far(t, r)

    load_ob.wait()

    def score_terms(t, pairs):
        z = None
        for i, r in pairs:
            term = dot(w2[i, 0:ZROWS, :], act[r, t])
            z = term if z is None else z + term
        return combine(z, right, left)

    outer_terms = ((0, ((0, 3),), ((0, 2), (1, 3)), 3), (1, ((2, 0),), ((1, 0), (2, 1)), 0))
    for t in range(OWN):
        for d, given, kept, r in outer_terms:
            main, tail_c = score_terms(t, given)
            kc[d, t, 0:64, :] = main
            kc[d, t, 64:72, :] = tail_c
            sp[d, t, 0:64, :] = main.astype(BF16)
            main, tail = score_terms(t, kept)
            main = main + bo[0:64, :]
            tail = tail + bo[64:72, :]
            sc[r, t, 0:64, :] = main
            sc[r, t, 64:72, :] = tail
            seen_main, seen_tail = parts(row_of(ob, t, r))
            sp[d, t, 64:128, :] = (main - seen_main).astype(BF16)
            sp[d, t, 128:144, :] = jnp.concatenate([tail_c, tail - seen_tail], axis=0).astype(BF16)
        for d, present in ((0, has_down), (1, has_up)):
            @pl.when(present)
            def _():
                x2_copy(d, t).start()

    def finish_row(t, r, main, tail):
        seen_main, seen_tail = parts(row_of(ob, t, r))
        stack_into(rs.at[r + 1, t], (main - seen_main).astype(BF16), tail - seen_tail, left, right)

    for t in range(OWN):
        for r in (1, 2):
            main, tail = score_terms(t, tuple((i, r + i - 1) for i in range(3)))
            main = main + bo[0:64, :]
            tail = tail + bo[64:72, :]
            put_row(so, t, r, main, tail)
            finish_row(t, r, main, tail)

    for d, r, halo, present in ((0, 0, 0, has_up), (1, 3, 5, has_down)):
        @pl.when(present)
        def _():
            for t in range(OWN):
                x2_copy(d, t).wait_recv()
                tails = rp[d, t, 128:144, :].astype(F32)
                sc[r, t, 0:64, :] += rp[d, t, 0:64, :].astype(F32)
                sc[r, t, 64:72, :] += tails[0:8]
                main = kc[1 - d, t, 0:64, :] + rp[d, t, 64:128, :].astype(F32)
                tail = kc[1 - d, t, 64:72, :] + tails[8:16]
                stack_into(rs.at[halo, t], main.astype(BF16), tail, left, right)

    for t in range(OWN):
        for r in (0, 3):
            finish_row(t, r, sc[r, t, 0:64, :], sc[r, t, 64:72, :])

    def grad_hidden(t, r):
        total = None
        for i in range(3):
            term = dot(w2t[i], rs[r + 2 - i, t])
            total = term if total is None else total + term
        gp[r + 1, t] = (total * slope[r, t]).astype(BF16)

    def hidden_inner(n, carry):
        grad_hidden(lax.rem(n, OWN), 1 + n // OWN)
        return carry

    for d, r, present in ((0, 3, has_down), (1, 0, has_up)):
        for t in range(OWN):
            grad_hidden(t, r)

        @pl.when(present)
        def _():
            x3_copy(d).start()

    for t in range(OWN):
        for r in (0, 3):
            put_row(so, t, r, sc[r, t, 0:64, :], sc[r, t, 64:72, :])

    lax.fori_loop(0, 2 * OWN, hidden_inner, 0, unroll=True)

    def grad_state(e, r, taps=(0, 1, 2)):
        z = None
        for t in range(OWN):
            k = e - t
            if 0 <= k < WINDOW:
                for i in taps:
                    term = dot(w4[i, k, 0:ZROWS, :], gp[r + 2 - i, t])
                    z = term if z is None else z + term
        return combine(z, left, right)

    sides = ((1, 0), (0, 4))

    def pack_row(d, r, pair):
        (main_a, tail_a), (main_b, tail_b) = pair
        sg[d, r, 0:64, :] = main_a.astype(BF16)
        sg[d, r, 64:80, :] = jnp.concatenate([tail_a, tail_b], axis=0).astype(BF16)
        sg[d, r, 80:144, :] = main_b.astype(BF16)

    def own_rows(rows):
        for r in rows:
            for s in range(OWN):
                main, tail = grad_state(OWN + s, r)
                own[r, s, 0:64, :] = main
                own[r, s, 64:72, :] = tail

    for r in (1, 2):
        for d, e in sides:
            pack_row(d, r, [grad_state(e + s, r) for s in range(OWN)])
    for r in (1, 2):
        for d, e in sides:
            g_copy(d, r).start()

    for n, (r, taps) in enumerate(((0, (0, 1)), (3, (1, 2)))):
        for d, e in sides:
            for s in range(OWN):
                main, tail = grad_state(e + s, r, taps)
                near[n, d, s, 0:64, :] = main
                near[n, d, s, 64:72, :] = tail
    own_rows((1, 2))

    for n, (r, tap, present) in enumerate(((0, 2, has_up), (3, 0, has_down))):
        @pl.when(present)
        def _():
            x3_copy(n).wait_recv()

        for d, e in sides:
            pair = []
            for s in range(OWN):
                main, tail = grad_state(e + s, r, (tap,))
                pair.append((main + near[n, d, s, 0:64, :], tail + near[n, d, s, 64:72, :]))
            pack_row(d, r, pair)
        for d, e in sides:
            g_copy(d, r).start()

    own_rows((0, 3))

    for d in range(2):
        remote(sbuf, rbuf.at[d], tm_send.at[d], tm_recv.at[d, 0, 0], (nxt, l)).wait_send()

        @pl.when(has_down if d == 0 else has_up)
        def _():
            remote(hb.at[d], hb.at[d], lat_send.at[d], lat_recv.at[d, 0], (nxt, l)).wait_send()
            for t in range(OWN):
                x2_copy(d, t).wait_send()
            x3_copy(d).wait_send()

    for r in (1, 2, 0, 3):
        g_copy(0, r).wait_recv()
        g_copy(1, r).wait_recv()
        tails = rg[0, r, 64:80, :].astype(F32) + rg[1, r, 64:80, :].astype(F32)
        for s in range(OWN):
            low = 80 * s
            main = own[r, s, 0:64, :] + rg[0, r, low : low + 64, :].astype(F32) + rg[1, r, low : low + 64, :].astype(F32)
            tail = own[r, s, 64:72, :] + tails[8 * s : 8 * s + 8]
            put_row(go, s, r, main, tail)

    for d in range(2):
        remote(sg.at[d], rg.at[d], g_send.at[d], g_recv.at[d, 0], (nxt, l)).wait_send()


def write_out(so, go, scores_out, guidance_out, sems):
    copies = []
    for s in range(OWN):
        copies.append(pltpu.make_async_copy(so.at[s], scores_out.at[s], sems.at[0, s]))
        copies.append(pltpu.make_async_copy(go.at[s], guidance_out.at[s], sems.at[1, s]))
    for copy in copies:
        copy.start()
    for copy in copies:
        copy.wait()


def solution(mesh):
    whole = P("tm", None, "lat", None)

    def step(states, observed, conv_in, bias_in, conv_out, bias_out):
        shape = states.shape
        dma = pltpu.SemaphoreType.DMA
        hbm = pl.BlockSpec(memory_space=pltpu.HBM)
        vmem = pl.BlockSpec(memory_space=pltpu.VMEM)
        view = (shape[0], shape[1] * shape[2] * 2, 128)

        def seen(x):
            halves = x.reshape(shape[0], shape[1], shape[2], 2, 128)
            return jnp.transpose(halves, (0, 1, 3, 2, 4)).reshape(view)

        def unseen(x):
            halves = x.reshape(shape[0], shape[1], 2, shape[2], 128)
            return jnp.transpose(halves, (0, 1, 3, 2, 4)).reshape(shape)

        so, go = pl.pallas_call(
            kernel,
            out_shape=(pltpu.VMEM(view, F32), pltpu.VMEM(view, F32)),
            in_specs=[hbm] * 6,
            out_specs=(vmem, vmem),
            scratch_shapes=[
                pltpu.VMEM(view, F32),
                pltpu.VMEM(view, F32),
                pltpu.VMEM((3, 3, WINDOW * C, HID), BF16),
                pltpu.VMEM((3, 3, C, HID), BF16),
                pltpu.VMEM((3, WINDOW, 256, HID), BF16),
                pltpu.VMEM((3, WINDOW, HID, 256), BF16),
                pltpu.VMEM((3, 256, HID), BF16),
                pltpu.VMEM((3, HID, 256), BF16),
                pltpu.VMEM((HID, LON), F32),
                pltpu.VMEM((MAIN + TAIL, LON), F32),
                pltpu.VMEM((OWN, 2, CHUNK, LON), BF16),
                pltpu.VMEM((2, OWN, 2, CHUNK, LON), BF16),
                pltpu.VMEM((2, SPAN, EDGE, LON), BF16),
                pltpu.VMEM((ROWS + 2, SPAN, 256, LON), BF16),
                pltpu.VMEM((OWN, ROWS, HID, LON), F32),
                pltpu.VMEM((ROWS, OWN, HID, LON), F32),
                pltpu.VMEM((ROWS, OWN, HID, LON), BF16),
                pltpu.VMEM((2, OWN, CHUNK, LON), BF16),
                pltpu.VMEM((2, OWN, CHUNK, LON), BF16),
                pltpu.VMEM((2, OWN, MAIN + TAIL, LON), F32),
                pltpu.VMEM((ROWS, OWN, MAIN + TAIL, LON), F32),
                pltpu.VMEM((ROWS + 2, OWN, 256, LON), BF16),
                pltpu.VMEM((ROWS + 2, OWN, HID, LON), BF16),
                pltpu.VMEM((2, ROWS, CHUNK, LON), BF16),
                pltpu.VMEM((2, ROWS, CHUNK, LON), BF16),
                pltpu.VMEM((ROWS, OWN, MAIN + TAIL, LON), F32),
                pltpu.VMEM((2, 2, OWN, MAIN + TAIL, LON), F32),
                pltpu.VMEM((HID,), F32),
                pltpu.VMEM((C,), F32),
                dma((6,)),
                dma((2,)),
                dma((2, OWN, 2)),
                dma((2,)),
                dma((2, SPAN)),
                dma((2, OWN)),
                dma((2, OWN)),
                dma((2,)),
                dma((2,)),
                dma((2,)),
                dma((2, ROWS)),
            ],
            compiler_params=pltpu.CompilerParams(
                collective_id=0, has_side_effects=True, vmem_limit_bytes=60 * 1024 * 1024
            ),
        )(seen(states), seen(observed), jnp.transpose(conv_in, (0, 1, 3, 2)), bias_in, conv_out, bias_out)
        so, go = (pltpu.with_memory_space_constraint(x, pltpu.VMEM) for x in (so, go))
        scores, guidance = pl.pallas_call(
            write_out,
            out_shape=(jax.ShapeDtypeStruct(view, F32), jax.ShapeDtypeStruct(view, F32)),
            in_specs=[vmem, vmem],
            out_specs=(hbm, hbm),
            scratch_shapes=[dma((2, OWN))],
            compiler_params=pltpu.CompilerParams(vmem_limit_bytes=4 * 1024 * 1024),
        )(so, go)
        return unseen(scores), unseen(guidance)

    sharded = jax.shard_map(
        step, mesh=mesh, in_specs=(whole, whole, P(), P(), P(), P()), out_specs=(whole, whole), check_vma=False
    )

    def run(*args):
        with jax.sharding.use_abstract_mesh(mesh.abstract_mesh):
            return sharded(*args)

    return run
```

```python
import jax
import jax.numpy as jnp
from jax import lax
from jax.experimental import pallas as pl
from jax.experimental.pallas import tpu as pltpu
from jax.sharding import PartitionSpec as P

MESH = pl.DeviceIdType.MESH
F32 = jnp.float32
BF16 = jnp.bfloat16
C = 69
HID = 256
WINDOW = 5
LON = 256
ROWS = 4
OWN = 2
SPAN = OWN + WINDOW - 1
MAIN = 64
TAIL = 8
STACK = 3 * (MAIN + TAIL)
ZROWS = 224
CHUNK = 2 * MAIN + 2 * TAIL
EDGE = MAIN + 2 * TAIL


def dot(a, b):
    return jnp.dot(a, b, preferred_element_type=F32)


def parts(x):
    tail = jnp.concatenate([x[MAIN:], jnp.zeros((MAIN + TAIL - C, x.shape[1]), F32)], axis=0)
    return x[:MAIN], tail


def row_of(ref, s, r):
    return jnp.concatenate([ref[s, pl.ds(ROWS * h + r, C, stride=2 * ROWS), :] for h in range(2)], axis=1)


def put_row(ref, s, r, main, tail):
    for h in range(2):
        lanes = slice(128 * h, 128 * h + 128)
        ref[s, pl.ds(ROWS * h + r, MAIN, stride=2 * ROWS), :] = main[:, lanes]
        ref[s, pl.ds(2 * ROWS * MAIN + ROWS * h + r, C - MAIN, stride=2 * ROWS), :] = tail[: C - MAIN, lanes]


def left(x):
    return pltpu.roll(x, LON - 1, axis=1)


def right(x):
    return pltpu.roll(x, 1, axis=1)


def stack_into(ref, main, tail, first, last):
    ref[0:64, :] = first(main)
    ref[64:128, :] = main
    ref[128:192, :] = last(main)
    tails = jnp.concatenate([first(tail), tail, last(tail), jnp.zeros((TAIL, LON), F32)], axis=0)
    ref[192:224, :] = tails.astype(BF16)


def combine(z, first, last):
    main = first(z[0:64]) + z[64:128] + last(z[128:192])
    tail = first(z[192:200]) + z[200:208] + last(z[208:216])
    return main, tail


def kernel(
    states, observed, conv_in, bias_in, conv_out, bias_out, so, go,
    st, ob, wi, wo, w4, w1, w2, w2t, bi, bo, sbuf, rbuf, hb, xs, pre, slope, act, sp, rp, kc, sc,
    rs, gp, sg, rg, own, near, b1, b2,
    local, tm_send, tm_recv, lat_send, lat_recv, x2_send, x2_recv, x3_send, x3_recv, g_send, g_recv,
):
    m = lax.axis_index("tm")
    l = lax.axis_index("lat")
    count_m = lax.axis_size("tm")
    count_l = lax.axis_size("lat")
    nxt = lax.rem(m + 1, count_m)
    prv = lax.rem(m + count_m - 1, count_m)
    has_up = l > 0
    has_down = l < count_l - 1

    load_st = pltpu.make_async_copy(states, st, local.at[0])
    load_wi = pltpu.make_async_copy(conv_in, wi, local.at[1])
    load_wo = pltpu.make_async_copy(conv_out, wo, local.at[2])
    load_ob = pltpu.make_async_copy(observed, ob, local.at[3])
    load_st.start()
    load_wi.start()
    load_wo.start()
    load_ob.start()
    load_b1 = pltpu.make_async_copy(bias_in, b1, local.at[4])
    load_b2 = pltpu.make_async_copy(bias_out, b2, local.at[5])
    load_b1.start()
    load_b2.start()

    barrier = pltpu.get_barrier_semaphore()
    pl.semaphore_signal(barrier, inc=1, device_id=(nxt, l), device_id_type=MESH)
    pl.semaphore_signal(barrier, inc=1, device_id=(prv, l), device_id_type=MESH)

    @pl.when(has_up)
    def _():
        pl.semaphore_signal(barrier, inc=1, device_id=(m, l - 1), device_id_type=MESH)

    @pl.when(has_down)
    def _():
        pl.semaphore_signal(barrier, inc=1, device_id=(m, l + 1), device_id_type=MESH)

    def remote(src, dst, send, recv, where):
        return pltpu.make_async_remote_copy(
            src_ref=src, dst_ref=dst, send_sem=send, recv_sem=recv, device_id=where, device_id_type=MESH
        )

    def tm_copy(d, s, g):
        where = (nxt, l) if d == 0 else (prv, l)
        return remote(sbuf.at[s, g], rbuf.at[d, s, g], tm_send.at[d], tm_recv.at[d, s, g], where)

    def lat_copy(d, e, chunk):
        if d == 0:
            return remote(chunk.at[pl.ds(MAIN, EDGE)], hb.at[0, e], lat_send.at[0], lat_recv.at[0, e], (m, l + 1))
        return remote(chunk.at[pl.ds(0, EDGE)], hb.at[1, e], lat_send.at[1], lat_recv.at[1, e], (m, l - 1))

    def chunk_of(e, g):
        if e < OWN:
            return rbuf.at[0, e, g]
        if e < 2 * OWN:
            return sbuf.at[e - OWN, g]
        return rbuf.at[1, e - 2 * OWN, g]

    def lat_start(e):
        @pl.when(has_down)
        def _():
            lat_copy(0, e, chunk_of(e, 0)).start()

        @pl.when(has_up)
        def _():
            lat_copy(1, e, chunk_of(e, 0)).start()

    def x2_copy(d, t):
        where = (m, l + 1) if d == 0 else (m, l - 1)
        return remote(sp.at[d, t], rp.at[d, t], x2_send.at[d, t], x2_recv.at[d, t], where)

    def x3_copy(d):
        if d == 0:
            return remote(gp.at[4], gp.at[0], x3_send.at[0], x3_recv.at[0], (m, l + 1))
        return remote(gp.at[1], gp.at[5], x3_send.at[1], x3_recv.at[1], (m, l - 1))

    def g_copy(d, r):
        where = (nxt, l) if d == 0 else (prv, l)
        return remote(sg.at[d, r], rg.at[d, r], g_send.at[d], g_recv.at[d, r], where)

    load_st.wait()
    for g, (a, b) in enumerate(((0, 3), (1, 2))):
        for s in range(OWN):
            main_a, tail_a = parts(row_of(st, s, a))
            main_b, tail_b = parts(row_of(st, s, b))
            sbuf[s, g, 0:64, :] = main_a.astype(BF16)
            sbuf[s, g, 64:80, :] = jnp.concatenate([tail_a, tail_b], axis=0).astype(BF16)
            sbuf[s, g, 80:144, :] = main_b.astype(BF16)
        if g == 0:
            pl.semaphore_wait(barrier, 2 + has_up.astype(jnp.int32) + has_down.astype(jnp.int32))

        tm_copy(0, 1, g).start()
        tm_copy(1, 0, g).start()
        tm_copy(0, 0, g).start()
        tm_copy(1, 1, g).start()
        if g == 0:
            for s in range(OWN):
                lat_start(OWN + s)

    def zero_pads(n, carry):
        xs[n // SPAN, lax.rem(n, SPAN), ZROWS:256, :] = jnp.zeros((256 - ZROWS, LON), BF16)
        return carry

    lax.fori_loop(0, (ROWS + 2) * SPAN, zero_pads, 0)
    for rho in range(ROWS + 2):
        for t in range(OWN):
            rs[rho, t, ZROWS:256, :] = jnp.zeros((256 - ZROWS, LON), BF16)

    def zero_halo(rho):
        def one(e, carry):
            xs[rho, e, 0:ZROWS, :] = jnp.zeros((ZROWS, LON), BF16)
            return carry

        lax.fori_loop(0, SPAN, one, 0)
        for t in range(OWN):
            rs[rho, t, 0:ZROWS, :] = jnp.zeros((ZROWS, LON), BF16)
            gp[rho, t] = jnp.zeros((HID, LON), BF16)

    @pl.when(jnp.logical_not(has_up))
    def _():
        zero_halo(0)

    @pl.when(jnp.logical_not(has_down))
    def _():
        zero_halo(ROWS + 1)

    load_b1.wait()
    load_b2.wait()
    bi[...] = jnp.broadcast_to(b1[...][None, :], (HID, HID)).T
    row = jnp.concatenate([b2[...][None, :], jnp.zeros((1, 128 - C), F32)], axis=1)
    column = jnp.broadcast_to(row, (128, 128)).T
    bo[...] = jnp.concatenate([column[: MAIN + TAIL], column[: MAIN + TAIL]], axis=1)

    load_wi.wait()

    def weights(i, carry):
        for k in range(WINDOW):
            tails = []
            for j in range(3):
                low = (C * k) // 16 * 16
                high = min((C * k + C + 15) // 16 * 16, WINDOW * C)
                piece = wi[i, j, low:high, :].astype(F32)[C * k - low : C * k - low + C]
                main, tail = parts(piece)
                w4[i, k, 64 * j : 64 * j + 64, :] = main.astype(BF16)
                tails.append(tail)
            tails.append(jnp.zeros((MAIN - 3 * TAIL, HID), F32))
            w4[i, k, 192:256, :] = jnp.concatenate(tails, axis=0).astype(BF16)
            w1[i, k] = w4[i, k].T
        return carry

    lax.fori_loop(0, 3, weights, 0)
    load_wo.wait()
    for i in range(3):
        tails = []
        for j in range(3):
            main, tail = parts(wo[i, j].astype(F32))
            w2[i, 64 * j : 64 * j + 64, :] = main.astype(BF16)
            tails.append(tail)
        tails.append(jnp.zeros((MAIN - 3 * TAIL, HID), F32))
        w2[i, 192:256, :] = jnp.concatenate(tails, axis=0).astype(BF16)
        w2t[i] = w2[i].T

    def stack_chunk(e, g):
        chunk = chunk_of(e, g)
        tails = chunk[64:80, :].astype(F32)
        a, b = ((0, 3), (1, 2))[g]
        stack_into(xs.at[a + 1, e], chunk[0:64, :], tails[0:8], right, left)
        stack_into(xs.at[b + 1, e], chunk[80:144, :], tails[8:16], right, left)

    def stack_halo(e):
        @pl.when(has_up)
        def _():
            lat_copy(0, e, chunk_of(e, 0)).wait_recv()
            stack_into(xs.at[0, e], hb[0, e, 16:80, :], hb[0, e, 0:16, :].astype(F32)[8:16], right, left)

        @pl.when(has_down)
        def _():
            lat_copy(1, e, chunk_of(e, 0)).wait_recv()
            stack_into(xs.at[5, e], hb[1, e, 0:64, :], hb[1, e, 64:80, :].astype(F32)[0:8], right, left)

    for s in range(OWN):
        stack_chunk(OWN + s, 0)
        stack_chunk(OWN + s, 1)

    inner = ((0, 1), (1, 1), (0, 2), (1, 2))
    outer = ((0, 0), (1, 0), (0, 3), (1, 3))
    edge = {0: (1,), 1: (0,), 2: (2,), 3: (1,)}
    rest = {0: (2, 0), 1: (1, 2), 2: (0, 1), 3: (0, 2)}

    def conv_states(t, r, total, picks, taps=(0, 1, 2)):
        for e in picks:
            for i in taps:
                total = total + dot(w1[i, e - t], xs[r + i, e])
        return total

    def phase_own(t, r):
        pre[t, r] = conv_states(t, r, bi[...], (2, 3))

    def phase_near(t, r):
        pre[t, r] = conv_states(t, r, pre[t, r], (1, 4), rest[r])

    def phase_far(t, r):
        v = conv_states(t, r, pre[t, r], (5 * t,), rest[r])
        sig = 0.5 + 0.5 * jnp.tanh(0.5 * v)
        act[r, t] = (v * sig).astype(BF16)
        slope[r, t] = sig * (1.0 + v * (1.0 - sig))

    for t, r in inner:
        phase_own(t, r)
    for s in range(OWN):
        stack_halo(OWN + s)
    for t, r in outer:
        phase_own(t, r)

    tm_copy(0, 1, 0).wait_recv()
    lat_start(1)
    tm_copy(1, 0, 0).wait_recv()
    lat_start(4)
    stack_chunk(1, 0)
    stack_chunk(4, 0)
    tm_copy(0, 0, 0).wait_recv()
    lat_start(0)
    tm_copy(1, 1, 0).wait_recv()
    lat_start(5)
    stack_chunk(0, 0)
    stack_chunk(5, 0)
    for t, r in inner + outer:
        pre[t, r] = conv_states(t, r, pre[t, r], (1, 4, 5 * t), edge[r])
    tm_copy(0, 1, 1).wait_recv()
    tm_copy(1, 0, 1).wait_recv()
    stack_chunk(1, 1)
    stack_chunk(4, 1)
    for t, r in inner:
        phase_near(t, r)
    stack_halo(1)
    stack_halo(4)
    for t, r in outer:
        phase_near(t, r)
    tm_copy(0, 0, 1).wait_recv()
    tm_copy(1, 1, 1).wait_recv()
    stack_chunk(0, 1)
    stack_chunk(5, 1)
    for t, r in inner:
        phase_far(t, r)
    stack_halo(0)
    stack_halo(5)
    for t, r in outer:
        phase_far(t, r)

    load_ob.wait()

    def score_terms(t, pairs):
        z = None
        for i, r in pairs:
            term = dot(w2[i, 0:ZROWS, :], act[r, t])
            z = term if z is None else z + term
        return combine(z, right, left)

    outer_terms = ((0, ((0, 3),), ((0, 2), (1, 3)), 3), (1, ((2, 0),), ((1, 0), (2, 1)), 0))
    for t in range(OWN):
        for d, given, kept, r in outer_terms:
            main, tail_c = score_terms(t, given)
            kc[d, t, 0:64, :] = main
            kc[d, t, 64:72, :] = tail_c
            sp[d, t, 0:64, :] = main.astype(BF16)
            main, tail = score_terms(t, kept)
            main = main + bo[0:64, :]
            tail = tail + bo[64:72, :]
            sc[r, t, 0:64, :] = main
            sc[r, t, 64:72, :] = tail
            seen_main, seen_tail = parts(row_of(ob, t, r))
            sp[d, t, 64:128, :] = (main - seen_main).astype(BF16)
            sp[d, t, 128:144, :] = jnp.concatenate([tail_c, tail - seen_tail], axis=0).astype(BF16)
        for d, present in ((0, has_down), (1, has_up)):
            @pl.when(present)
            def _():
                x2_copy(d, t).start()

    def finish_row(t, r, main, tail):
        seen_main, seen_tail = parts(row_of(ob, t, r))
        stack_into(rs.at[r + 1, t], (main - seen_main).astype(BF16), tail - seen_tail, left, right)

    for t in range(OWN):
        for r in (1, 2):
            main, tail = score_terms(t, tuple((i, r + i - 1) for i in range(3)))
            main = main + bo[0:64, :]
            tail = tail + bo[64:72, :]
            put_row(so, t, r, main, tail)
            finish_row(t, r, main, tail)

    for d, r, halo, present in ((0, 0, 0, has_up), (1, 3, 5, has_down)):
        @pl.when(present)
        def _():
            for t in range(OWN):
                x2_copy(d, t).wait_recv()
                tails = rp[d, t, 128:144, :].astype(F32)
                sc[r, t, 0:64, :] += rp[d, t, 0:64, :].astype(F32)
                sc[r, t, 64:72, :] += tails[0:8]
                main = kc[1 - d, t, 0:64, :] + rp[d, t, 64:128, :].astype(F32)
                tail = kc[1 - d, t, 64:72, :] + tails[8:16]
                stack_into(rs.at[halo, t], main.astype(BF16), tail, left, right)

    for t in range(OWN):
        for r in (0, 3):
            finish_row(t, r, sc[r, t, 0:64, :], sc[r, t, 64:72, :])

    def grad_hidden(t, r):
        total = None
        for i in range(3):
            term = dot(w2t[i], rs[r + 2 - i, t])
            total = term if total is None else total + term
        gp[r + 1, t] = (total * slope[r, t]).astype(BF16)

    def hidden_inner(n, carry):
        grad_hidden(lax.rem(n, OWN), 1 + n // OWN)
        return carry

    for d, r, present in ((0, 3, has_down), (1, 0, has_up)):
        for t in range(OWN):
            grad_hidden(t, r)

        @pl.when(present)
        def _():
            x3_copy(d).start()

    for t in range(OWN):
        for r in (0, 3):
            put_row(so, t, r, sc[r, t, 0:64, :], sc[r, t, 64:72, :])

    lax.fori_loop(0, 2 * OWN, hidden_inner, 0, unroll=True)

    def grad_state(e, r, taps=(0, 1, 2)):
        z = None
        for t in range(OWN):
            k = e - t
            if 0 <= k < WINDOW:
                for i in taps:
                    term = dot(w4[i, k, 0:ZROWS, :], gp[r + 2 - i, t])
                    z = term if z is None else z + term
        return combine(z, left, right)

    sides = ((1, 0), (0, 4))

    def pack_row(d, r, pair):
        (main_a, tail_a), (main_b, tail_b) = pair
        sg[d, r, 0:64, :] = main_a.astype(BF16)
        sg[d, r, 64:80, :] = jnp.concatenate([tail_a, tail_b], axis=0).astype(BF16)
        sg[d, r, 80:144, :] = main_b.astype(BF16)

    def own_rows(rows):
        for r in rows:
            for s in range(OWN):
                main, tail = grad_state(OWN + s, r)
                own[r, s, 0:64, :] = main
                own[r, s, 64:72, :] = tail

    for r in (1, 2):
        for d, e in sides:
            pack_row(d, r, [grad_state(e + s, r) for s in range(OWN)])
        for d, e in sides:
            g_copy(d, r).start()

    for n, (r, taps) in enumerate(((0, (0, 1)), (3, (1, 2)))):
        for d, e in sides:
            for s in range(OWN):
                main, tail = grad_state(e + s, r, taps)
                near[n, d, s, 0:64, :] = main
                near[n, d, s, 64:72, :] = tail
    own_rows((1, 2))

    for n, (r, tap, present) in enumerate(((0, 2, has_up), (3, 0, has_down))):
        @pl.when(present)
        def _():
            x3_copy(n).wait_recv()

        for d, e in sides:
            pair = []
            for s in range(OWN):
                main, tail = grad_state(e + s, r, (tap,))
                pair.append((main + near[n, d, s, 0:64, :], tail + near[n, d, s, 64:72, :]))
            pack_row(d, r, pair)
        for d, e in sides:
            g_copy(d, r).start()

    own_rows((0, 3))

    for d in range(2):
        remote(sbuf, rbuf.at[d], tm_send.at[d], tm_recv.at[d, 0, 0], (nxt, l)).wait_send()

        @pl.when(has_down if d == 0 else has_up)
        def _():
            remote(hb.at[d], hb.at[d], lat_send.at[d], lat_recv.at[d, 0], (nxt, l)).wait_send()
            for t in range(OWN):
                x2_copy(d, t).wait_send()
            x3_copy(d).wait_send()

    for r in (1, 2, 0, 3):
        g_copy(0, r).wait_recv()
        g_copy(1, r).wait_recv()
        tails = rg[0, r, 64:80, :].astype(F32) + rg[1, r, 64:80, :].astype(F32)
        for s in range(OWN):
            low = 80 * s
            main = own[r, s, 0:64, :] + rg[0, r, low : low + 64, :].astype(F32) + rg[1, r, low : low + 64, :].astype(F32)
            tail = own[r, s, 64:72, :] + tails[8 * s : 8 * s + 8]
            put_row(go, s, r, main, tail)

    for d in range(2):
        remote(sg.at[d], rg.at[d], g_send.at[d], g_recv.at[d, 0], (nxt, l)).wait_send()


def write_out(so, go, scores_out, guidance_out, sems):
    copies = []
    for s in range(OWN):
        copies.append(pltpu.make_async_copy(so.at[s], scores_out.at[s], sems.at[0, s]))
        copies.append(pltpu.make_async_copy(go.at[s], guidance_out.at[s], sems.at[1, s]))
    for copy in copies:
        copy.start()
    for copy in copies:
        copy.wait()


def solution(mesh):
    whole = P("tm", None, "lat", None)

    def step(states, observed, conv_in, bias_in, conv_out, bias_out):
        shape = states.shape
        dma = pltpu.SemaphoreType.DMA
        hbm = pl.BlockSpec(memory_space=pltpu.HBM)
        vmem = pl.BlockSpec(memory_space=pltpu.VMEM)
        view = (shape[0], shape[1] * shape[2] * 2, 128)

        def seen(x):
            halves = x.reshape(shape[0], shape[1], shape[2], 2, 128)
            return jnp.transpose(halves, (0, 1, 3, 2, 4)).reshape(view)

        def unseen(x):
            halves = x.reshape(shape[0], shape[1], 2, shape[2], 128)
            return jnp.transpose(halves, (0, 1, 3, 2, 4)).reshape(shape)

        so, go = pl.pallas_call(
            kernel,
            out_shape=(pltpu.VMEM(view, F32), pltpu.VMEM(view, F32)),
            in_specs=[hbm] * 6,
            out_specs=(vmem, vmem),
            scratch_shapes=[
                pltpu.VMEM(view, F32),
                pltpu.VMEM(view, F32),
                pltpu.VMEM((3, 3, WINDOW * C, HID), BF16),
                pltpu.VMEM((3, 3, C, HID), BF16),
                pltpu.VMEM((3, WINDOW, 256, HID), BF16),
                pltpu.VMEM((3, WINDOW, HID, 256), BF16),
                pltpu.VMEM((3, 256, HID), BF16),
                pltpu.VMEM((3, HID, 256), BF16),
                pltpu.VMEM((HID, LON), F32),
                pltpu.VMEM((MAIN + TAIL, LON), F32),
                pltpu.VMEM((OWN, 2, CHUNK, LON), BF16),
                pltpu.VMEM((2, OWN, 2, CHUNK, LON), BF16),
                pltpu.VMEM((2, SPAN, EDGE, LON), BF16),
                pltpu.VMEM((ROWS + 2, SPAN, 256, LON), BF16),
                pltpu.VMEM((OWN, ROWS, HID, LON), F32),
                pltpu.VMEM((ROWS, OWN, HID, LON), F32),
                pltpu.VMEM((ROWS, OWN, HID, LON), BF16),
                pltpu.VMEM((2, OWN, CHUNK, LON), BF16),
                pltpu.VMEM((2, OWN, CHUNK, LON), BF16),
                pltpu.VMEM((2, OWN, MAIN + TAIL, LON), F32),
                pltpu.VMEM((ROWS, OWN, MAIN + TAIL, LON), F32),
                pltpu.VMEM((ROWS + 2, OWN, 256, LON), BF16),
                pltpu.VMEM((ROWS + 2, OWN, HID, LON), BF16),
                pltpu.VMEM((2, ROWS, CHUNK, LON), BF16),
                pltpu.VMEM((2, ROWS, CHUNK, LON), BF16),
                pltpu.VMEM((ROWS, OWN, MAIN + TAIL, LON), F32),
                pltpu.VMEM((2, 2, OWN, MAIN + TAIL, LON), F32),
                pltpu.VMEM((HID,), F32),
                pltpu.VMEM((C,), F32),
                dma((6,)),
                dma((2,)),
                dma((2, OWN, 2)),
                dma((2,)),
                dma((2, SPAN)),
                dma((2, OWN)),
                dma((2, OWN)),
                dma((2,)),
                dma((2,)),
                dma((2,)),
                dma((2, ROWS)),
            ],
            compiler_params=pltpu.CompilerParams(
                collective_id=0, has_side_effects=True, vmem_limit_bytes=60 * 1024 * 1024
            ),
        )(seen(states), seen(observed), jnp.transpose(conv_in, (0, 1, 3, 2)), bias_in, conv_out, bias_out)
        so, go = (pltpu.with_memory_space_constraint(x, pltpu.VMEM) for x in (so, go))
        scores, guidance = pl.pallas_call(
            write_out,
            out_shape=(jax.ShapeDtypeStruct(view, F32), jax.ShapeDtypeStruct(view, F32)),
            in_specs=[vmem, vmem],
            out_specs=(hbm, hbm),
            scratch_shapes=[dma((2, OWN))],
            compiler_params=pltpu.CompilerParams(vmem_limit_bytes=4 * 1024 * 1024),
        )(so, go)
        return unseen(scores), unseen(guidance)

    sharded = jax.shard_map(
        step, mesh=mesh, in_specs=(whole, whole, P(), P(), P(), P()), out_specs=(whole, whole), check_vma=False
    )

    def run(*args):
        with jax.sharding.use_abstract_mesh(mesh.abstract_mesh):
            return sharded(*args)

    return run
```

```python
import jax
import jax.numpy as jnp
from jax import lax
from jax.experimental import pallas as pl
from jax.experimental.pallas import tpu as pltpu
from jax.sharding import PartitionSpec as P

MESH = pl.DeviceIdType.MESH
F32 = jnp.float32
BF16 = jnp.bfloat16
C = 69
HID = 256
WINDOW = 5
LON = 256
ROWS = 4
OWN = 2
SPAN = OWN + WINDOW - 1
MAIN = 64
TAIL = 8
STACK = 3 * (MAIN + TAIL)
ZROWS = 224
CHUNK = 2 * MAIN + 2 * TAIL
EDGE = MAIN + 2 * TAIL


def dot(a, b):
    return jnp.dot(a, b, preferred_element_type=F32)


def parts(x):
    tail = jnp.concatenate([x[MAIN:], jnp.zeros((MAIN + TAIL - C, x.shape[1]), F32)], axis=0)
    return x[:MAIN], tail


def row_of(ref, s, r):
    return jnp.concatenate([ref[s, pl.ds(ROWS * h + r, C, stride=2 * ROWS), :] for h in range(2)], axis=1)


def put_row(ref, s, r, main, tail):
    for h in range(2):
        lanes = slice(128 * h, 128 * h + 128)
        ref[s, pl.ds(ROWS * h + r, MAIN, stride=2 * ROWS), :] = main[:, lanes]
        ref[s, pl.ds(2 * ROWS * MAIN + ROWS * h + r, C - MAIN, stride=2 * ROWS), :] = tail[: C - MAIN, lanes]


def left(x):
    return pltpu.roll(x, LON - 1, axis=1)


def right(x):
    return pltpu.roll(x, 1, axis=1)


def stack_into(ref, main, tail, first, last):
    ref[0:64, :] = first(main)
    ref[64:128, :] = main
    ref[128:192, :] = last(main)
    tails = jnp.concatenate([first(tail), tail, last(tail), jnp.zeros((TAIL, LON), F32)], axis=0)
    ref[192:224, :] = tails.astype(BF16)


def combine(z, first, last):
    main = first(z[0:64]) + z[64:128] + last(z[128:192])
    tail = first(z[192:200]) + z[200:208] + last(z[208:216])
    return main, tail


def kernel(
    states, observed, conv_in, bias_in, conv_out, bias_out, so, go,
    st, ob, wi, wo, w4, w1, w2, w2t, bi, bo, sbuf, rbuf, hb, xs, pre, slope, act, sp, rp, kc, sc,
    rs, gp, sg, rg, own, near, b1, b2,
    local, tm_send, tm_recv, lat_send, lat_recv, x2_send, x2_recv, x3_send, x3_recv, g_send, g_recv,
):
    m = lax.axis_index("tm")
    l = lax.axis_index("lat")
    count_m = lax.axis_size("tm")
    count_l = lax.axis_size("lat")
    nxt = lax.rem(m + 1, count_m)
    prv = lax.rem(m + count_m - 1, count_m)
    has_up = l > 0
    has_down = l < count_l - 1

    load_st = pltpu.make_async_copy(states, st, local.at[0])
    load_wi = pltpu.make_async_copy(conv_in, wi, local.at[1])
    load_wo = pltpu.make_async_copy(conv_out, wo, local.at[2])
    load_ob = pltpu.make_async_copy(observed, ob, local.at[3])
    load_st.start()
    load_wi.start()
    load_wo.start()
    load_ob.start()
    load_b1 = pltpu.make_async_copy(bias_in, b1, local.at[4])
    load_b2 = pltpu.make_async_copy(bias_out, b2, local.at[5])
    load_b1.start()
    load_b2.start()

    barrier = pltpu.get_barrier_semaphore()
    pl.semaphore_signal(barrier, inc=1, device_id=(nxt, l), device_id_type=MESH)
    pl.semaphore_signal(barrier, inc=1, device_id=(prv, l), device_id_type=MESH)

    @pl.when(has_up)
    def _():
        pl.semaphore_signal(barrier, inc=1, device_id=(m, l - 1), device_id_type=MESH)

    @pl.when(has_down)
    def _():
        pl.semaphore_signal(barrier, inc=1, device_id=(m, l + 1), device_id_type=MESH)

    def remote(src, dst, send, recv, where):
        return pltpu.make_async_remote_copy(
            src_ref=src, dst_ref=dst, send_sem=send, recv_sem=recv, device_id=where, device_id_type=MESH
        )

    def tm_copy(d, s, g):
        where = (nxt, l) if d == 0 else (prv, l)
        return remote(sbuf.at[s, g], rbuf.at[d, s, g], tm_send.at[d], tm_recv.at[d, s, g], where)

    def lat_copy(d, e, chunk):
        if d == 0:
            return remote(chunk.at[pl.ds(MAIN, EDGE)], hb.at[0, e], lat_send.at[0], lat_recv.at[0, e], (m, l + 1))
        return remote(chunk.at[pl.ds(0, EDGE)], hb.at[1, e], lat_send.at[1], lat_recv.at[1, e], (m, l - 1))

    def chunk_of(e, g):
        if e < OWN:
            return rbuf.at[0, e, g]
        if e < 2 * OWN:
            return sbuf.at[e - OWN, g]
        return rbuf.at[1, e - 2 * OWN, g]

    def lat_start(e):
        @pl.when(has_down)
        def _():
            lat_copy(0, e, chunk_of(e, 0)).start()

        @pl.when(has_up)
        def _():
            lat_copy(1, e, chunk_of(e, 0)).start()

    def x2_copy(d, t):
        where = (m, l + 1) if d == 0 else (m, l - 1)
        return remote(sp.at[d, t], rp.at[d, t], x2_send.at[d, t], x2_recv.at[d, t], where)

    def x3_copy(d):
        if d == 0:
            return remote(gp.at[4], gp.at[0], x3_send.at[0], x3_recv.at[0], (m, l + 1))
        return remote(gp.at[1], gp.at[5], x3_send.at[1], x3_recv.at[1], (m, l - 1))

    def g_copy(d, r):
        where = (nxt, l) if d == 0 else (prv, l)
        return remote(sg.at[d, r], rg.at[d, r], g_send.at[d], g_recv.at[d, r], where)

    load_st.wait()
    for g, (a, b) in enumerate(((0, 3), (1, 2))):
        for s in range(OWN):
            main_a, tail_a = parts(row_of(st, s, a))
            main_b, tail_b = parts(row_of(st, s, b))
            sbuf[s, g, 0:64, :] = main_a.astype(BF16)
            sbuf[s, g, 64:80, :] = jnp.concatenate([tail_a, tail_b], axis=0).astype(BF16)
            sbuf[s, g, 80:144, :] = main_b.astype(BF16)
        if g == 0:
            pl.semaphore_wait(barrier, 2 + has_up.astype(jnp.int32) + has_down.astype(jnp.int32))

        tm_copy(0, 1, g).start()
        tm_copy(1, 0, g).start()
        tm_copy(0, 0, g).start()
        tm_copy(1, 1, g).start()
        if g == 0:
            for s in range(OWN):
                lat_start(OWN + s)

    def zero_pads(n, carry):
        xs[n // SPAN, lax.rem(n, SPAN), ZROWS:256, :] = jnp.zeros((256 - ZROWS, LON), BF16)
        return carry

    lax.fori_loop(0, (ROWS + 2) * SPAN, zero_pads, 0)
    for rho in range(ROWS + 2):
        for t in range(OWN):
            rs[rho, t, ZROWS:256, :] = jnp.zeros((256 - ZROWS, LON), BF16)

    def zero_halo(rho):
        def one(e, carry):
            xs[rho, e, 0:ZROWS, :] = jnp.zeros((ZROWS, LON), BF16)
            return carry

        lax.fori_loop(0, SPAN, one, 0)
        for t in range(OWN):
            rs[rho, t, 0:ZROWS, :] = jnp.zeros((ZROWS, LON), BF16)
            gp[rho, t] = jnp.zeros((HID, LON), BF16)

    @pl.when(jnp.logical_not(has_up))
    def _():
        zero_halo(0)

    @pl.when(jnp.logical_not(has_down))
    def _():
        zero_halo(ROWS + 1)

    load_b1.wait()
    load_b2.wait()
    bi[...] = jnp.broadcast_to(b1[...][None, :], (HID, HID)).T
    row = jnp.concatenate([b2[...][None, :], jnp.zeros((1, 128 - C), F32)], axis=1)
    column = jnp.broadcast_to(row, (128, 128)).T
    bo[...] = jnp.concatenate([column[: MAIN + TAIL], column[: MAIN + TAIL]], axis=1)

    load_wi.wait()

    def weights(i, carry):
        for k in range(WINDOW):
            tails = []
            for j in range(3):
                low = (C * k) // 16 * 16
                high = min((C * k + C + 15) // 16 * 16, WINDOW * C)
                piece = wi[i, j, low:high, :].astype(F32)[C * k - low : C * k - low + C]
                main, tail = parts(piece)
                w4[i, k, 64 * j : 64 * j + 64, :] = main.astype(BF16)
                tails.append(tail)
            tails.append(jnp.zeros((MAIN - 3 * TAIL, HID), F32))
            w4[i, k, 192:256, :] = jnp.concatenate(tails, axis=0).astype(BF16)
            w1[i, k] = w4[i, k].T
        return carry

    lax.fori_loop(0, 3, weights, 0)
    load_wo.wait()
    for i in range(3):
        tails = []
        for j in range(3):
            main, tail = parts(wo[i, j].astype(F32))
            w2[i, 64 * j : 64 * j + 64, :] = main.astype(BF16)
            tails.append(tail)
        tails.append(jnp.zeros((MAIN - 3 * TAIL, HID), F32))
        w2[i, 192:256, :] = jnp.concatenate(tails, axis=0).astype(BF16)
        w2t[i] = w2[i].T

    def stack_chunk(e, g):
        chunk = chunk_of(e, g)
        tails = chunk[64:80, :].astype(F32)
        a, b = ((0, 3), (1, 2))[g]
        stack_into(xs.at[a + 1, e], chunk[0:64, :], tails[0:8], right, left)
        stack_into(xs.at[b + 1, e], chunk[80:144, :], tails[8:16], right, left)

    def stack_halo(e):
        @pl.when(has_up)
        def _():
            lat_copy(0, e, chunk_of(e, 0)).wait_recv()
            stack_into(xs.at[0, e], hb[0, e, 16:80, :], hb[0, e, 0:16, :].astype(F32)[8:16], right, left)

        @pl.when(has_down)
        def _():
            lat_copy(1, e, chunk_of(e, 0)).wait_recv()
            stack_into(xs.at[5, e], hb[1, e, 0:64, :], hb[1, e, 64:80, :].astype(F32)[0:8], right, left)

    for s in range(OWN):
        stack_chunk(OWN + s, 0)
        stack_chunk(OWN + s, 1)

    inner = ((0, 1), (1, 1), (0, 2), (1, 2))
    outer = ((0, 0), (1, 0), (0, 3), (1, 3))
    edge = {0: (1,), 1: (0,), 2: (2,), 3: (1,)}
    rest = {0: (2, 0), 1: (1, 2), 2: (0, 1), 3: (0, 2)}

    def conv_states(t, r, total, picks, taps=(0, 1, 2)):
        for e in picks:
            for i in taps:
                total = total + dot(w1[i, e - t], xs[r + i, e])
        return total

    def phase_own(t, r):
        pre[t, r] = conv_states(t, r, bi[...], (2, 3))

    def phase_near(t, r):
        pre[t, r] = conv_states(t, r, pre[t, r], (1, 4), rest[r])

    def phase_far(t, r):
        v = conv_states(t, r, pre[t, r], (5 * t,), rest[r])
        sig = 0.5 + 0.5 * jnp.tanh(0.5 * v)
        act[r, t] = (v * sig).astype(BF16)
        slope[r, t] = sig * (1.0 + v * (1.0 - sig))

    for t, r in inner:
        phase_own(t, r)
    for s in range(OWN):
        stack_halo(OWN + s)
    for t, r in outer:
        phase_own(t, r)

    tm_copy(0, 1, 0).wait_recv()
    lat_start(1)
    tm_copy(1, 0, 0).wait_recv()
    lat_start(4)
    stack_chunk(1, 0)
    stack_chunk(4, 0)
    tm_copy(0, 0, 0).wait_recv()
    lat_start(0)
    tm_copy(1, 1, 0).wait_recv()
    lat_start(5)
    stack_chunk(0, 0)
    stack_chunk(5, 0)
    for t, r in inner + outer:
        pre[t, r] = conv_states(t, r, pre[t, r], (1, 4, 5 * t), edge[r])
    stack_halo(1)
    stack_halo(4)
    tm_copy(0, 1, 1).wait_recv()
    tm_copy(1, 0, 1).wait_recv()
    stack_chunk(1, 1)
    stack_chunk(4, 1)
    for t, r in inner + outer:
        phase_near(t, r)
    load_ob.wait()
    stack_halo(0)
    stack_halo(5)
    tm_copy(0, 0, 1).wait_recv()
    tm_copy(1, 1, 1).wait_recv()
    stack_chunk(0, 1)
    stack_chunk(5, 1)
    for t in range(OWN):
        for r in (0, 1, 3, 2):
            phase_far(t, r)

    def score_terms(t, pairs):
        z = None
        for i, r in pairs:
            term = dot(w2[i, 0:ZROWS, :], act[r, t])
            z = term if z is None else z + term
        return combine(z, right, left)

    outer_terms = ((0, ((0, 3),), ((0, 2), (1, 3)), 3), (1, ((2, 0),), ((1, 0), (2, 1)), 0))
    for t in range(OWN):
        for d, given, kept, r in outer_terms:
            main, tail_c = score_terms(t, given)
            kc[d, t, 0:64, :] = main
            kc[d, t, 64:72, :] = tail_c
            sp[d, t, 0:64, :] = main.astype(BF16)
            main, tail = score_terms(t, kept)
            main = main + bo[0:64, :]
            tail = tail + bo[64:72, :]
            sc[r, t, 0:64, :] = main
            sc[r, t, 64:72, :] = tail
            seen_main, seen_tail = parts(row_of(ob, t, r))
            sp[d, t, 64:128, :] = (main - seen_main).astype(BF16)
            sp[d, t, 128:144, :] = jnp.concatenate([tail_c, tail - seen_tail], axis=0).astype(BF16)
        for d, present in ((0, has_down), (1, has_up)):
            @pl.when(present)
            def _():
                x2_copy(d, t).start()

    def finish_row(t, r, main, tail):
        seen_main, seen_tail = parts(row_of(ob, t, r))
        stack_into(rs.at[r + 1, t], (main - seen_main).astype(BF16), tail - seen_tail, left, right)

    for t in range(OWN):
        for r in (1, 2):
            main, tail = score_terms(t, tuple((i, r + i - 1) for i in range(3)))
            main = main + bo[0:64, :]
            tail = tail + bo[64:72, :]
            put_row(so, t, r, main, tail)
            finish_row(t, r, main, tail)

    for d, r, halo, present in ((0, 0, 0, has_up), (1, 3, 5, has_down)):
        @pl.when(present)
        def _():
            for t in range(OWN):
                x2_copy(d, t).wait_recv()
                tails = rp[d, t, 128:144, :].astype(F32)
                sc[r, t, 0:64, :] += rp[d, t, 0:64, :].astype(F32)
                sc[r, t, 64:72, :] += tails[0:8]
                main = kc[1 - d, t, 0:64, :] + rp[d, t, 64:128, :].astype(F32)
                tail = kc[1 - d, t, 64:72, :] + tails[8:16]
                stack_into(rs.at[halo, t], main.astype(BF16), tail, left, right)

    for t in range(OWN):
        for r in (0, 3):
            finish_row(t, r, sc[r, t, 0:64, :], sc[r, t, 64:72, :])

    def grad_hidden(t, r):
        total = None
        for i in range(3):
            term = dot(w2t[i], rs[r + 2 - i, t])
            total = term if total is None else total + term
        gp[r + 1, t] = (total * slope[r, t]).astype(BF16)

    def hidden_inner(n, carry):
        grad_hidden(lax.rem(n, OWN), 1 + n // OWN)
        return carry

    for d, r, present in ((0, 3, has_down), (1, 0, has_up)):
        for t in range(OWN):
            grad_hidden(t, r)

        @pl.when(present)
        def _():
            x3_copy(d).start()

    lax.fori_loop(0, 2 * OWN, hidden_inner, 0, unroll=True)

    def grad_state(e, r, taps=(0, 1, 2)):
        z = None
        for t in range(OWN):
            k = e - t
            if 0 <= k < WINDOW:
                for i in taps:
                    term = dot(w4[i, k, 0:ZROWS, :], gp[r + 2 - i, t])
                    z = term if z is None else z + term
        return combine(z, left, right)

    sides = ((1, 0), (0, 4))

    def pack_row(d, r, pair):
        (main_a, tail_a), (main_b, tail_b) = pair
        sg[d, r, 0:64, :] = main_a.astype(BF16)
        sg[d, r, 64:80, :] = jnp.concatenate([tail_a, tail_b], axis=0).astype(BF16)
        sg[d, r, 80:144, :] = main_b.astype(BF16)

    def own_rows(rows):
        for r in rows:
            for s in range(OWN):
                main, tail = grad_state(OWN + s, r)
                own[r, s, 0:64, :] = main
                own[r, s, 64:72, :] = tail

    for r in (1, 2):
        for d, e in sides:
            pack_row(d, r, [grad_state(e + s, r) for s in range(OWN)])
        for d, e in sides:
            g_copy(d, r).start()

    for t in range(OWN):
        for r in (0, 3):
            put_row(so, t, r, sc[r, t, 0:64, :], sc[r, t, 64:72, :])

    for n, (r, taps) in enumerate(((0, (0, 1)), (3, (1, 2)))):
        for d, e in sides:
            for s in range(OWN):
                main, tail = grad_state(e + s, r, taps)
                near[n, d, s, 0:64, :] = main
                near[n, d, s, 64:72, :] = tail
    own_rows((1, 2))

    for n, (r, tap, present) in enumerate(((0, 2, has_up), (3, 0, has_down))):
        @pl.when(present)
        def _():
            x3_copy(n).wait_recv()

        for d, e in sides:
            pair = []
            for s in range(OWN):
                main, tail = grad_state(e + s, r, (tap,))
                pair.append((main + near[n, d, s, 0:64, :], tail + near[n, d, s, 64:72, :]))
            pack_row(d, r, pair)
        for d, e in sides:
            g_copy(d, r).start()

    own_rows((0, 3))

    for d in range(2):
        remote(sbuf, rbuf.at[d], tm_send.at[d], tm_recv.at[d, 0, 0], (nxt, l)).wait_send()

        @pl.when(has_down if d == 0 else has_up)
        def _():
            remote(hb.at[d], hb.at[d], lat_send.at[d], lat_recv.at[d, 0], (nxt, l)).wait_send()
            for t in range(OWN):
                x2_copy(d, t).wait_send()
            x3_copy(d).wait_send()

    for r in (1, 2, 0, 3):
        g_copy(0, r).wait_recv()
        g_copy(1, r).wait_recv()
        tails = rg[0, r, 64:80, :].astype(F32) + rg[1, r, 64:80, :].astype(F32)
        for s in range(OWN):
            low = 80 * s
            main = own[r, s, 0:64, :] + rg[0, r, low : low + 64, :].astype(F32) + rg[1, r, low : low + 64, :].astype(F32)
            tail = own[r, s, 64:72, :] + tails[8 * s : 8 * s + 8]
            put_row(go, s, r, main, tail)

    for d in range(2):
        remote(sg.at[d], rg.at[d], g_send.at[d], g_recv.at[d, 0], (nxt, l)).wait_send()


def write_out(so, go, scores_out, guidance_out, sems):
    copies = []
    for s in range(OWN):
        copies.append(pltpu.make_async_copy(so.at[s], scores_out.at[s], sems.at[0, s]))
        copies.append(pltpu.make_async_copy(go.at[s], guidance_out.at[s], sems.at[1, s]))
    for copy in copies:
        copy.start()
    for copy in copies:
        copy.wait()


def solution(mesh):
    whole = P("tm", None, "lat", None)

    def step(states, observed, conv_in, bias_in, conv_out, bias_out):
        shape = states.shape
        dma = pltpu.SemaphoreType.DMA
        hbm = pl.BlockSpec(memory_space=pltpu.HBM)
        vmem = pl.BlockSpec(memory_space=pltpu.VMEM)
        view = (shape[0], shape[1] * shape[2] * 2, 128)

        def seen(x):
            halves = x.reshape(shape[0], shape[1], shape[2], 2, 128)
            return jnp.transpose(halves, (0, 1, 3, 2, 4)).reshape(view)

        def unseen(x):
            halves = x.reshape(shape[0], shape[1], 2, shape[2], 128)
            return jnp.transpose(halves, (0, 1, 3, 2, 4)).reshape(shape)

        so, go = pl.pallas_call(
            kernel,
            out_shape=(pltpu.VMEM(view, F32), pltpu.VMEM(view, F32)),
            in_specs=[hbm] * 6,
            out_specs=(vmem, vmem),
            scratch_shapes=[
                pltpu.VMEM(view, F32),
                pltpu.VMEM(view, F32),
                pltpu.VMEM((3, 3, WINDOW * C, HID), BF16),
                pltpu.VMEM((3, 3, C, HID), BF16),
                pltpu.VMEM((3, WINDOW, 256, HID), BF16),
                pltpu.VMEM((3, WINDOW, HID, 256), BF16),
                pltpu.VMEM((3, 256, HID), BF16),
                pltpu.VMEM((3, HID, 256), BF16),
                pltpu.VMEM((HID, LON), F32),
                pltpu.VMEM((MAIN + TAIL, LON), F32),
                pltpu.VMEM((OWN, 2, CHUNK, LON), BF16),
                pltpu.VMEM((2, OWN, 2, CHUNK, LON), BF16),
                pltpu.VMEM((2, SPAN, EDGE, LON), BF16),
                pltpu.VMEM((ROWS + 2, SPAN, 256, LON), BF16),
                pltpu.VMEM((OWN, ROWS, HID, LON), F32),
                pltpu.VMEM((ROWS, OWN, HID, LON), F32),
                pltpu.VMEM((ROWS, OWN, HID, LON), BF16),
                pltpu.VMEM((2, OWN, CHUNK, LON), BF16),
                pltpu.VMEM((2, OWN, CHUNK, LON), BF16),
                pltpu.VMEM((2, OWN, MAIN + TAIL, LON), F32),
                pltpu.VMEM((ROWS, OWN, MAIN + TAIL, LON), F32),
                pltpu.VMEM((ROWS + 2, OWN, 256, LON), BF16),
                pltpu.VMEM((ROWS + 2, OWN, HID, LON), BF16),
                pltpu.VMEM((2, ROWS, CHUNK, LON), BF16),
                pltpu.VMEM((2, ROWS, CHUNK, LON), BF16),
                pltpu.VMEM((ROWS, OWN, MAIN + TAIL, LON), F32),
                pltpu.VMEM((2, 2, OWN, MAIN + TAIL, LON), F32),
                pltpu.VMEM((HID,), F32),
                pltpu.VMEM((C,), F32),
                dma((6,)),
                dma((2,)),
                dma((2, OWN, 2)),
                dma((2,)),
                dma((2, SPAN)),
                dma((2, OWN)),
                dma((2, OWN)),
                dma((2,)),
                dma((2,)),
                dma((2,)),
                dma((2, ROWS)),
            ],
            compiler_params=pltpu.CompilerParams(
                collective_id=0, has_side_effects=True, vmem_limit_bytes=60 * 1024 * 1024
            ),
        )(seen(states), seen(observed), jnp.transpose(conv_in, (0, 1, 3, 2)), bias_in, conv_out, bias_out)
        so, go = (pltpu.with_memory_space_constraint(x, pltpu.VMEM) for x in (so, go))
        scores, guidance = pl.pallas_call(
            write_out,
            out_shape=(jax.ShapeDtypeStruct(view, F32), jax.ShapeDtypeStruct(view, F32)),
            in_specs=[vmem, vmem],
            out_specs=(hbm, hbm),
            scratch_shapes=[dma((2, OWN))],
            compiler_params=pltpu.CompilerParams(vmem_limit_bytes=4 * 1024 * 1024),
        )(so, go)
        return unseen(scores), unseen(guidance)

    sharded = jax.shard_map(
        step, mesh=mesh, in_specs=(whole, whole, P(), P(), P(), P()), out_specs=(whole, whole), check_vma=False
    )

    def run(*args):
        with jax.sharding.use_abstract_mesh(mesh.abstract_mesh):
            return sharded(*args)

    return run
```

```python
import jax
import jax.numpy as jnp
from jax import lax
from jax.experimental import pallas as pl
from jax.experimental.pallas import tpu as pltpu
from jax.sharding import PartitionSpec as P

MESH = pl.DeviceIdType.MESH
F32 = jnp.float32
BF16 = jnp.bfloat16
C = 69
HID = 256
WINDOW = 5
LON = 256
ROWS = 4
OWN = 2
SPAN = OWN + WINDOW - 1
MAIN = 64
TAIL = 8
STACK = 3 * (MAIN + TAIL)
ZROWS = 224
CHUNK = 2 * MAIN + 2 * TAIL
EDGE = MAIN + 2 * TAIL


def dot(a, b):
    return jnp.dot(a, b, preferred_element_type=F32)


def parts(x):
    tail = jnp.concatenate([x[MAIN:], jnp.zeros((MAIN + TAIL - C, x.shape[1]), F32)], axis=0)
    return x[:MAIN], tail


def row_of(ref, s, r):
    return jnp.concatenate([ref[s, pl.ds(ROWS * h + r, C, stride=2 * ROWS), :] for h in range(2)], axis=1)


def put_row(ref, s, r, main, tail):
    for h in range(2):
        lanes = slice(128 * h, 128 * h + 128)
        ref[s, pl.ds(ROWS * h + r, MAIN, stride=2 * ROWS), :] = main[:, lanes]
        ref[s, pl.ds(2 * ROWS * MAIN + ROWS * h + r, C - MAIN, stride=2 * ROWS), :] = tail[: C - MAIN, lanes]


def left(x):
    return pltpu.roll(x, LON - 1, axis=1)


def right(x):
    return pltpu.roll(x, 1, axis=1)


def stack_into(ref, main, tail, first, last):
    ref[0:64, :] = first(main)
    ref[64:128, :] = main
    ref[128:192, :] = last(main)
    tails = jnp.concatenate([first(tail), tail, last(tail), jnp.zeros((TAIL, LON), F32)], axis=0)
    ref[192:224, :] = tails.astype(BF16)


def combine(z, first, last):
    main = first(z[0:64]) + z[64:128] + last(z[128:192])
    tail = first(z[192:200]) + z[200:208] + last(z[208:216])
    return main, tail


def kernel(
    states, observed, conv_in, bias_in, conv_out, bias_out, so, go,
    st, ob, wi, wo, w4, w1, w2, w2t, bi, bo, sbuf, rbuf, hb, xs, pre, slope, act, sp, rp, kc, sc,
    rs, gp, sg, rg, own, near, b1, b2,
    local, tm_send, tm_recv, lat_send, lat_recv, x2_send, x2_recv, x3_send, x3_recv, g_send, g_recv,
):
    m = lax.axis_index("tm")
    l = lax.axis_index("lat")
    count_m = lax.axis_size("tm")
    count_l = lax.axis_size("lat")
    nxt = lax.rem(m + 1, count_m)
    prv = lax.rem(m + count_m - 1, count_m)
    has_up = l > 0
    has_down = l < count_l - 1

    load_st = pltpu.make_async_copy(states, st, local.at[0])
    load_wi = pltpu.make_async_copy(conv_in, wi, local.at[1])
    load_wo = pltpu.make_async_copy(conv_out, wo, local.at[2])
    load_ob = pltpu.make_async_copy(observed, ob, local.at[3])
    load_st.start()
    load_wi.start()
    load_wo.start()
    load_ob.start()
    load_b1 = pltpu.make_async_copy(bias_in, b1, local.at[4])
    load_b2 = pltpu.make_async_copy(bias_out, b2, local.at[5])
    load_b1.start()
    load_b2.start()

    barrier = pltpu.get_barrier_semaphore()
    pl.semaphore_signal(barrier, inc=1, device_id=(nxt, l), device_id_type=MESH)
    pl.semaphore_signal(barrier, inc=1, device_id=(prv, l), device_id_type=MESH)

    @pl.when(has_up)
    def _():
        pl.semaphore_signal(barrier, inc=1, device_id=(m, l - 1), device_id_type=MESH)

    @pl.when(has_down)
    def _():
        pl.semaphore_signal(barrier, inc=1, device_id=(m, l + 1), device_id_type=MESH)

    def remote(src, dst, send, recv, where):
        return pltpu.make_async_remote_copy(
            src_ref=src, dst_ref=dst, send_sem=send, recv_sem=recv, device_id=where, device_id_type=MESH
        )

    def tm_copy(d, s, g):
        where = (nxt, l) if d == 0 else (prv, l)
        return remote(sbuf.at[s, g], rbuf.at[d, s, g], tm_send.at[d], tm_recv.at[d, s, g], where)

    def lat_copy(d, e, chunk):
        if d == 0:
            return remote(chunk.at[pl.ds(MAIN, EDGE)], hb.at[0, e], lat_send.at[0], lat_recv.at[0, e], (m, l + 1))
        return remote(chunk.at[pl.ds(0, EDGE)], hb.at[1, e], lat_send.at[1], lat_recv.at[1, e], (m, l - 1))

    def chunk_of(e, g):
        if e < OWN:
            return rbuf.at[0, e, g]
        if e < 2 * OWN:
            return sbuf.at[e - OWN, g]
        return rbuf.at[1, e - 2 * OWN, g]

    def lat_start(e):
        @pl.when(has_down)
        def _():
            lat_copy(0, e, chunk_of(e, 0)).start()

        @pl.when(has_up)
        def _():
            lat_copy(1, e, chunk_of(e, 0)).start()

    def x2_copy(d, t):
        where = (m, l + 1) if d == 0 else (m, l - 1)
        return remote(sp.at[d, t], rp.at[d, t], x2_send.at[d, t], x2_recv.at[d, t], where)

    def x3_copy(d, t):
        if d == 0:
            return remote(gp.at[4, t], gp.at[0, t], x3_send.at[0, t], x3_recv.at[0, t], (m, l + 1))
        return remote(gp.at[1, t], gp.at[5, t], x3_send.at[1, t], x3_recv.at[1, t], (m, l - 1))

    def g_copy(d, r):
        where = (nxt, l) if d == 0 else (prv, l)
        return remote(sg.at[d, r], rg.at[d, r], g_send.at[d], g_recv.at[d, r], where)

    load_st.wait()
    for g, (a, b) in enumerate(((0, 3), (1, 2))):
        for s in range(OWN):
            main_a, tail_a = parts(row_of(st, s, a))
            main_b, tail_b = parts(row_of(st, s, b))
            sbuf[s, g, 0:64, :] = main_a.astype(BF16)
            sbuf[s, g, 64:80, :] = jnp.concatenate([tail_a, tail_b], axis=0).astype(BF16)
            sbuf[s, g, 80:144, :] = main_b.astype(BF16)
        if g == 0:
            pl.semaphore_wait(barrier, 2 + has_up.astype(jnp.int32) + has_down.astype(jnp.int32))

        tm_copy(0, 1, g).start()
        tm_copy(1, 0, g).start()
        tm_copy(0, 0, g).start()
        tm_copy(1, 1, g).start()
        if g == 0:
            for s in range(OWN):
                lat_start(OWN + s)

    def zero_pads(n, carry):
        xs[n // SPAN, lax.rem(n, SPAN), ZROWS:256, :] = jnp.zeros((256 - ZROWS, LON), BF16)
        return carry

    lax.fori_loop(0, (ROWS + 2) * SPAN, zero_pads, 0)
    for rho in range(ROWS + 2):
        for t in range(OWN):
            rs[rho, t, ZROWS:256, :] = jnp.zeros((256 - ZROWS, LON), BF16)

    def zero_halo(rho):
        def one(e, carry):
            xs[rho, e, 0:ZROWS, :] = jnp.zeros((ZROWS, LON), BF16)
            return carry

        lax.fori_loop(0, SPAN, one, 0)
        for t in range(OWN):
            rs[rho, t, 0:ZROWS, :] = jnp.zeros((ZROWS, LON), BF16)
            gp[rho, t] = jnp.zeros((HID, LON), BF16)

    @pl.when(jnp.logical_not(has_up))
    def _():
        zero_halo(0)

    @pl.when(jnp.logical_not(has_down))
    def _():
        zero_halo(ROWS + 1)

    load_b1.wait()
    load_b2.wait()
    bi[...] = jnp.broadcast_to(b1[...][None, :], (HID, HID)).T
    row = jnp.concatenate([b2[...][None, :], jnp.zeros((1, 128 - C), F32)], axis=1)
    column = jnp.broadcast_to(row, (128, 128)).T
    bo[...] = jnp.concatenate([column[: MAIN + TAIL], column[: MAIN + TAIL]], axis=1)

    load_wi.wait()

    def weights(i, carry):
        for k in range(WINDOW):
            tails = []
            for j in range(3):
                low = (C * k) // 16 * 16
                high = min((C * k + C + 15) // 16 * 16, WINDOW * C)
                piece = wi[i, j, low:high, :].astype(F32)[C * k - low : C * k - low + C]
                main, tail = parts(piece)
                w4[i, k, 64 * j : 64 * j + 64, :] = main.astype(BF16)
                tails.append(tail)
            tails.append(jnp.zeros((MAIN - 3 * TAIL, HID), F32))
            w4[i, k, 192:256, :] = jnp.concatenate(tails, axis=0).astype(BF16)
            w1[i, k] = w4[i, k].T
        return carry

    lax.fori_loop(0, 3, weights, 0)
    load_wo.wait()
    for i in range(3):
        tails = []
        for j in range(3):
            main, tail = parts(wo[i, j].astype(F32))
            w2[i, 64 * j : 64 * j + 64, :] = main.astype(BF16)
            tails.append(tail)
        tails.append(jnp.zeros((MAIN - 3 * TAIL, HID), F32))
        w2[i, 192:256, :] = jnp.concatenate(tails, axis=0).astype(BF16)
        w2t[i] = w2[i].T

    def stack_chunk(e, g):
        chunk = chunk_of(e, g)
        tails = chunk[64:80, :].astype(F32)
        a, b = ((0, 3), (1, 2))[g]
        stack_into(xs.at[a + 1, e], chunk[0:64, :], tails[0:8], right, left)
        stack_into(xs.at[b + 1, e], chunk[80:144, :], tails[8:16], right, left)

    def stack_halo(e):
        @pl.when(has_up)
        def _():
            lat_copy(0, e, chunk_of(e, 0)).wait_recv()
            stack_into(xs.at[0, e], hb[0, e, 16:80, :], hb[0, e, 0:16, :].astype(F32)[8:16], right, left)

        @pl.when(has_down)
        def _():
            lat_copy(1, e, chunk_of(e, 0)).wait_recv()
            stack_into(xs.at[5, e], hb[1, e, 0:64, :], hb[1, e, 64:80, :].astype(F32)[0:8], right, left)

    for s in range(OWN):
        stack_chunk(OWN + s, 0)
        stack_chunk(OWN + s, 1)

    inner = ((0, 1), (1, 1), (0, 2), (1, 2))
    outer = ((0, 0), (1, 0), (0, 3), (1, 3))
    edge = {0: (1,), 1: (0,), 2: (2,), 3: (1,)}
    rest = {0: (2, 0), 1: (1, 2), 2: (0, 1), 3: (0, 2)}

    def conv_states(t, r, total, picks, taps=(0, 1, 2)):
        for e in picks:
            for i in taps:
                total = total + dot(w1[i, e - t], xs[r + i, e])
        return total

    def phase_own(t, r):
        pre[t, r] = conv_states(t, r, bi[...], (2, 3))

    def phase_near(t, r):
        pre[t, r] = conv_states(t, r, pre[t, r], (1, 4), rest[r])

    def phase_far(t, r):
        v = conv_states(t, r, pre[t, r], (5 * t,), rest[r])
        sig = 0.5 + 0.5 * jnp.tanh(0.5 * v)
        act[r, t] = (v * sig).astype(BF16)
        slope[r, t] = sig * (1.0 + v * (1.0 - sig))

    for t, r in inner:
        phase_own(t, r)
    for s in range(OWN):
        stack_halo(OWN + s)
    for t, r in outer:
        phase_own(t, r)

    tm_copy(0, 1, 0).wait_recv()
    lat_start(1)
    tm_copy(1, 0, 0).wait_recv()
    lat_start(4)
    stack_chunk(1, 0)
    stack_chunk(4, 0)
    tm_copy(0, 0, 0).wait_recv()
    lat_start(0)
    tm_copy(1, 1, 0).wait_recv()
    lat_start(5)
    stack_chunk(0, 0)
    stack_chunk(5, 0)
    for t, r in inner + outer:
        pre[t, r] = conv_states(t, r, pre[t, r], (1, 4, 5 * t), edge[r])
    tm_copy(0, 1, 1).wait_recv()
    tm_copy(1, 0, 1).wait_recv()
    stack_chunk(1, 1)
    stack_chunk(4, 1)
    for t, r in inner:
        phase_near(t, r)
    stack_halo(1)
    stack_halo(4)
    for t, r in outer:
        phase_near(t, r)
    load_ob.wait()
    stack_halo(0)
    stack_halo(5)
    tm_copy(0, 0, 1).wait_recv()
    tm_copy(1, 1, 1).wait_recv()
    stack_chunk(0, 1)
    stack_chunk(5, 1)
    for t in range(OWN):
        for r in (0, 1, 3, 2):
            phase_far(t, r)

    def score_terms(t, pairs):
        z = None
        for i, r in pairs:
            term = dot(w2[i, 0:ZROWS, :], act[r, t])
            z = term if z is None else z + term
        return combine(z, right, left)

    outer_terms = ((0, ((0, 3),), ((0, 2), (1, 3)), 3), (1, ((2, 0),), ((1, 0), (2, 1)), 0))
    for t in range(OWN):
        for d, given, kept, r in outer_terms:
            main, tail_c = score_terms(t, given)
            kc[d, t, 0:64, :] = main
            kc[d, t, 64:72, :] = tail_c
            sp[d, t, 0:64, :] = main.astype(BF16)
            main, tail = score_terms(t, kept)
            main = main + bo[0:64, :]
            tail = tail + bo[64:72, :]
            sc[r, t, 0:64, :] = main
            sc[r, t, 64:72, :] = tail
            seen_main, seen_tail = parts(row_of(ob, t, r))
            sp[d, t, 64:128, :] = (main - seen_main).astype(BF16)
            sp[d, t, 128:144, :] = jnp.concatenate([tail_c, tail - seen_tail], axis=0).astype(BF16)
        for d, present in ((0, has_down), (1, has_up)):
            @pl.when(present)
            def _():
                x2_copy(d, t).start()

    def finish_row(t, r, main, tail):
        seen_main, seen_tail = parts(row_of(ob, t, r))
        stack_into(rs.at[r + 1, t], (main - seen_main).astype(BF16), tail - seen_tail, left, right)

    for t in range(OWN):
        for r in (1, 2):
            main, tail = score_terms(t, tuple((i, r + i - 1) for i in range(3)))
            main = main + bo[0:64, :]
            tail = tail + bo[64:72, :]
            put_row(so, t, r, main, tail)
            finish_row(t, r, main, tail)

    for d, r, halo, present in ((0, 0, 0, has_up), (1, 3, 5, has_down)):
        @pl.when(present)
        def _():
            for t in range(OWN):
                x2_copy(d, t).wait_recv()
                tails = rp[d, t, 128:144, :].astype(F32)
                sc[r, t, 0:64, :] += rp[d, t, 0:64, :].astype(F32)
                sc[r, t, 64:72, :] += tails[0:8]
                main = kc[1 - d, t, 0:64, :] + rp[d, t, 64:128, :].astype(F32)
                tail = kc[1 - d, t, 64:72, :] + tails[8:16]
                stack_into(rs.at[halo, t], main.astype(BF16), tail, left, right)

    for t in range(OWN):
        for r in (0, 3):
            finish_row(t, r, sc[r, t, 0:64, :], sc[r, t, 64:72, :])

    def grad_hidden(t, r):
        total = None
        for i in range(3):
            term = dot(w2t[i], rs[r + 2 - i, t])
            total = term if total is None else total + term
        gp[r + 1, t] = (total * slope[r, t]).astype(BF16)

    def hidden_inner(n, carry):
        grad_hidden(lax.rem(n, OWN), 1 + n // OWN)
        return carry

    for t in range(OWN):
        for d, r, present in ((0, 3, has_down), (1, 0, has_up)):
            grad_hidden(t, r)

            @pl.when(present)
            def _():
                x3_copy(d, t).start()

    lax.fori_loop(0, 2 * OWN, hidden_inner, 0, unroll=True)

    def grad_state(e, r, taps=(0, 1, 2)):
        z = None
        for t in range(OWN):
            k = e - t
            if 0 <= k < WINDOW:
                for i in taps:
                    term = dot(w4[i, k, 0:ZROWS, :], gp[r + 2 - i, t])
                    z = term if z is None else z + term
        return combine(z, left, right)

    sides = ((1, 0), (0, 4))

    def pack_row(d, r, pair):
        (main_a, tail_a), (main_b, tail_b) = pair
        sg[d, r, 0:64, :] = main_a.astype(BF16)
        sg[d, r, 64:80, :] = jnp.concatenate([tail_a, tail_b], axis=0).astype(BF16)
        sg[d, r, 80:144, :] = main_b.astype(BF16)

    def own_rows(rows):
        for r in rows:
            for s in range(OWN):
                main, tail = grad_state(OWN + s, r)
                own[r, s, 0:64, :] = main
                own[r, s, 64:72, :] = tail

    for r in (1, 2):
        for d, e in sides:
            pack_row(d, r, [grad_state(e + s, r) for s in range(OWN)])
        for d, e in sides:
            g_copy(d, r).start()

    for t in range(OWN):
        for r in (0, 3):
            put_row(so, t, r, sc[r, t, 0:64, :], sc[r, t, 64:72, :])

    for n, (r, taps) in enumerate(((0, (0, 1)), (3, (1, 2)))):
        for d, e in sides:
            for s in range(OWN):
                main, tail = grad_state(e + s, r, taps)
                near[n, d, s, 0:64, :] = main
                near[n, d, s, 64:72, :] = tail
    own_rows((1, 2))

    for n, (r, tap, present) in enumerate(((0, 2, has_up), (3, 0, has_down))):
        @pl.when(present)
        def _():
            for t in range(OWN):
                x3_copy(n, t).wait_recv()

        for d, e in sides:
            pair = []
            for s in range(OWN):
                main, tail = grad_state(e + s, r, (tap,))
                pair.append((main + near[n, d, s, 0:64, :], tail + near[n, d, s, 64:72, :]))
            pack_row(d, r, pair)
        for d, e in sides:
            g_copy(d, r).start()

    own_rows((0, 3))

    for d in range(2):
        remote(sbuf, rbuf.at[d], tm_send.at[d], tm_recv.at[d, 0, 0], (nxt, l)).wait_send()

        @pl.when(has_down if d == 0 else has_up)
        def _():
            remote(hb.at[d], hb.at[d], lat_send.at[d], lat_recv.at[d, 0], (nxt, l)).wait_send()
            for t in range(OWN):
                x2_copy(d, t).wait_send()
                x3_copy(d, t).wait_send()

    for r in (1, 2, 0, 3):
        g_copy(0, r).wait_recv()
        g_copy(1, r).wait_recv()
        tails = rg[0, r, 64:80, :].astype(F32) + rg[1, r, 64:80, :].astype(F32)
        for s in range(OWN):
            low = 80 * s
            main = own[r, s, 0:64, :] + rg[0, r, low : low + 64, :].astype(F32) + rg[1, r, low : low + 64, :].astype(F32)
            tail = own[r, s, 64:72, :] + tails[8 * s : 8 * s + 8]
            put_row(go, s, r, main, tail)

    for d in range(2):
        remote(sg.at[d], rg.at[d], g_send.at[d], g_recv.at[d, 0], (nxt, l)).wait_send()


def write_out(so, go, scores_out, guidance_out, sems):
    copies = []
    for s in range(OWN):
        copies.append(pltpu.make_async_copy(so.at[s], scores_out.at[s], sems.at[0, s]))
        copies.append(pltpu.make_async_copy(go.at[s], guidance_out.at[s], sems.at[1, s]))
    for copy in copies:
        copy.start()
    for copy in copies:
        copy.wait()


def solution(mesh):
    whole = P("tm", None, "lat", None)

    def step(states, observed, conv_in, bias_in, conv_out, bias_out):
        shape = states.shape
        dma = pltpu.SemaphoreType.DMA
        hbm = pl.BlockSpec(memory_space=pltpu.HBM)
        vmem = pl.BlockSpec(memory_space=pltpu.VMEM)
        view = (shape[0], shape[1] * shape[2] * 2, 128)

        def seen(x):
            halves = x.reshape(shape[0], shape[1], shape[2], 2, 128)
            return jnp.transpose(halves, (0, 1, 3, 2, 4)).reshape(view)

        def unseen(x):
            halves = x.reshape(shape[0], shape[1], 2, shape[2], 128)
            return jnp.transpose(halves, (0, 1, 3, 2, 4)).reshape(shape)

        so, go = pl.pallas_call(
            kernel,
            out_shape=(pltpu.VMEM(view, F32), pltpu.VMEM(view, F32)),
            in_specs=[hbm] * 6,
            out_specs=(vmem, vmem),
            scratch_shapes=[
                pltpu.VMEM(view, F32),
                pltpu.VMEM(view, F32),
                pltpu.VMEM((3, 3, WINDOW * C, HID), BF16),
                pltpu.VMEM((3, 3, C, HID), BF16),
                pltpu.VMEM((3, WINDOW, 256, HID), BF16),
                pltpu.VMEM((3, WINDOW, HID, 256), BF16),
                pltpu.VMEM((3, 256, HID), BF16),
                pltpu.VMEM((3, HID, 256), BF16),
                pltpu.VMEM((HID, LON), F32),
                pltpu.VMEM((MAIN + TAIL, LON), F32),
                pltpu.VMEM((OWN, 2, CHUNK, LON), BF16),
                pltpu.VMEM((2, OWN, 2, CHUNK, LON), BF16),
                pltpu.VMEM((2, SPAN, EDGE, LON), BF16),
                pltpu.VMEM((ROWS + 2, SPAN, 256, LON), BF16),
                pltpu.VMEM((OWN, ROWS, HID, LON), F32),
                pltpu.VMEM((ROWS, OWN, HID, LON), F32),
                pltpu.VMEM((ROWS, OWN, HID, LON), BF16),
                pltpu.VMEM((2, OWN, CHUNK, LON), BF16),
                pltpu.VMEM((2, OWN, CHUNK, LON), BF16),
                pltpu.VMEM((2, OWN, MAIN + TAIL, LON), F32),
                pltpu.VMEM((ROWS, OWN, MAIN + TAIL, LON), F32),
                pltpu.VMEM((ROWS + 2, OWN, 256, LON), BF16),
                pltpu.VMEM((ROWS + 2, OWN, HID, LON), BF16),
                pltpu.VMEM((2, ROWS, CHUNK, LON), BF16),
                pltpu.VMEM((2, ROWS, CHUNK, LON), BF16),
                pltpu.VMEM((ROWS, OWN, MAIN + TAIL, LON), F32),
                pltpu.VMEM((2, 2, OWN, MAIN + TAIL, LON), F32),
                pltpu.VMEM((HID,), F32),
                pltpu.VMEM((C,), F32),
                dma((6,)),
                dma((2,)),
                dma((2, OWN, 2)),
                dma((2,)),
                dma((2, SPAN)),
                dma((2, OWN)),
                dma((2, OWN)),
                dma((2, OWN)),
                dma((2, OWN)),
                dma((2,)),
                dma((2, ROWS)),
            ],
            compiler_params=pltpu.CompilerParams(
                collective_id=0, has_side_effects=True, vmem_limit_bytes=60 * 1024 * 1024
            ),
        )(seen(states), seen(observed), jnp.transpose(conv_in, (0, 1, 3, 2)), bias_in, conv_out, bias_out)
        so, go = (pltpu.with_memory_space_constraint(x, pltpu.VMEM) for x in (so, go))
        scores, guidance = pl.pallas_call(
            write_out,
            out_shape=(jax.ShapeDtypeStruct(view, F32), jax.ShapeDtypeStruct(view, F32)),
            in_specs=[vmem, vmem],
            out_specs=(hbm, hbm),
            scratch_shapes=[dma((2, OWN))],
            compiler_params=pltpu.CompilerParams(vmem_limit_bytes=4 * 1024 * 1024),
        )(so, go)
        return unseen(scores), unseen(guidance)

    sharded = jax.shard_map(
        step, mesh=mesh, in_specs=(whole, whole, P(), P(), P(), P()), out_specs=(whole, whole), check_vma=False
    )

    def run(*args):
        with jax.sharding.use_abstract_mesh(mesh.abstract_mesh):
            return sharded(*args)

    return run
```

```python
import jax
import jax.numpy as jnp
from jax import lax
from jax.experimental import pallas as pl
from jax.experimental.pallas import tpu as pltpu
from jax.sharding import PartitionSpec as P

MESH = pl.DeviceIdType.MESH
F32 = jnp.float32
BF16 = jnp.bfloat16
C = 69
HID = 256
WINDOW = 5
LON = 256
ROWS = 4
OWN = 2
SPAN = OWN + WINDOW - 1
MAIN = 64
TAIL = 8
STACK = 3 * (MAIN + TAIL)
ZROWS = 224
CHUNK = 2 * MAIN + 2 * TAIL
EDGE = MAIN + 2 * TAIL


def dot(a, b):
    return jnp.dot(a, b, preferred_element_type=F32)


def parts(x):
    tail = jnp.concatenate([x[MAIN:], jnp.zeros((MAIN + TAIL - C, x.shape[1]), F32)], axis=0)
    return x[:MAIN], tail


def row_of(ref, s, r):
    return jnp.concatenate([ref[s, pl.ds(ROWS * h + r, C, stride=2 * ROWS), :] for h in range(2)], axis=1)


def put_row(ref, s, r, main, tail):
    for h in range(2):
        lanes = slice(128 * h, 128 * h + 128)
        ref[s, pl.ds(ROWS * h + r, MAIN, stride=2 * ROWS), :] = main[:, lanes]
        ref[s, pl.ds(2 * ROWS * MAIN + ROWS * h + r, C - MAIN, stride=2 * ROWS), :] = tail[: C - MAIN, lanes]


def left(x):
    return pltpu.roll(x, LON - 1, axis=1)


def right(x):
    return pltpu.roll(x, 1, axis=1)


def stack_into(ref, main, tail, first, last):
    ref[0:64, :] = first(main)
    ref[64:128, :] = main
    ref[128:192, :] = last(main)
    tails = jnp.concatenate([first(tail), tail, last(tail), jnp.zeros((TAIL, LON), F32)], axis=0)
    ref[192:224, :] = tails.astype(BF16)


def combine(z, first, last):
    main = first(z[0:64]) + z[64:128] + last(z[128:192])
    tail = first(z[192:200]) + z[200:208] + last(z[208:216])
    return main, tail


def kernel(
    states, observed, conv_in, bias_in, conv_out, bias_out, so, go,
    st, ob, wi, wo, w4, w1, w2, w2t, bi, bo, sbuf, rbuf, hb, xs, pre, slope, act, sp, rp, kc, sc,
    rs, gp, sg, rg, own, near, b1, b2,
    local, tm_send, tm_recv, lat_send, lat_recv, x2_send, x2_recv, x3_send, x3_recv, g_send, g_recv,
):
    m = lax.axis_index("tm")
    l = lax.axis_index("lat")
    count_m = lax.axis_size("tm")
    count_l = lax.axis_size("lat")
    nxt = lax.rem(m + 1, count_m)
    prv = lax.rem(m + count_m - 1, count_m)
    has_up = l > 0
    has_down = l < count_l - 1

    load_st = pltpu.make_async_copy(states, st, local.at[0])
    load_wi = pltpu.make_async_copy(conv_in, wi, local.at[1])
    load_wo = pltpu.make_async_copy(conv_out, wo, local.at[2])
    load_ob = pltpu.make_async_copy(observed, ob, local.at[3])
    load_st.start()
    load_wi.start()
    load_wo.start()
    load_ob.start()
    load_b1 = pltpu.make_async_copy(bias_in, b1, local.at[4])
    load_b2 = pltpu.make_async_copy(bias_out, b2, local.at[5])
    load_b1.start()
    load_b2.start()

    barrier = pltpu.get_barrier_semaphore()
    pl.semaphore_signal(barrier, inc=1, device_id=(nxt, l), device_id_type=MESH)
    pl.semaphore_signal(barrier, inc=1, device_id=(prv, l), device_id_type=MESH)

    @pl.when(has_up)
    def _():
        pl.semaphore_signal(barrier, inc=1, device_id=(m, l - 1), device_id_type=MESH)

    @pl.when(has_down)
    def _():
        pl.semaphore_signal(barrier, inc=1, device_id=(m, l + 1), device_id_type=MESH)

    def remote(src, dst, send, recv, where):
        return pltpu.make_async_remote_copy(
            src_ref=src, dst_ref=dst, send_sem=send, recv_sem=recv, device_id=where, device_id_type=MESH
        )

    def tm_copy(d, s, g):
        where = (nxt, l) if d == 0 else (prv, l)
        return remote(sbuf.at[s, g], rbuf.at[d, s, g], tm_send.at[d], tm_recv.at[d, s, g], where)

    def lat_copy(d, e, chunk):
        if d == 0:
            return remote(chunk.at[pl.ds(MAIN, EDGE)], hb.at[0, e], lat_send.at[0], lat_recv.at[0, e], (m, l + 1))
        return remote(chunk.at[pl.ds(0, EDGE)], hb.at[1, e], lat_send.at[1], lat_recv.at[1, e], (m, l - 1))

    def chunk_of(e, g):
        if e < OWN:
            return rbuf.at[0, e, g]
        if e < 2 * OWN:
            return sbuf.at[e - OWN, g]
        return rbuf.at[1, e - 2 * OWN, g]

    def lat_start(e):
        @pl.when(has_down)
        def _():
            lat_copy(0, e, chunk_of(e, 0)).start()

        @pl.when(has_up)
        def _():
            lat_copy(1, e, chunk_of(e, 0)).start()

    def x2_copy(d, t):
        where = (m, l + 1) if d == 0 else (m, l - 1)
        return remote(sp.at[d, t], rp.at[d, t], x2_send.at[d, t], x2_recv.at[d, t], where)

    def x3_copy(d, t):
        if d == 0:
            return remote(gp.at[4, t], gp.at[0, t], x3_send.at[0, t], x3_recv.at[0, t], (m, l + 1))
        return remote(gp.at[1, t], gp.at[5, t], x3_send.at[1, t], x3_recv.at[1, t], (m, l - 1))

    def g_copy(d, r):
        where = (nxt, l) if d == 0 else (prv, l)
        return remote(sg.at[d, r], rg.at[d, r], g_send.at[d], g_recv.at[d, r], where)

    load_st.wait()
    for g, (a, b) in enumerate(((0, 3), (1, 2))):
        for s in range(OWN):
            main_a, tail_a = parts(row_of(st, s, a))
            main_b, tail_b = parts(row_of(st, s, b))
            sbuf[s, g, 0:64, :] = main_a.astype(BF16)
            sbuf[s, g, 64:80, :] = jnp.concatenate([tail_a, tail_b], axis=0).astype(BF16)
            sbuf[s, g, 80:144, :] = main_b.astype(BF16)
        if g == 0:
            pl.semaphore_wait(barrier, 2 + has_up.astype(jnp.int32) + has_down.astype(jnp.int32))

        tm_copy(0, 1, g).start()
        tm_copy(1, 0, g).start()
        tm_copy(0, 0, g).start()
        tm_copy(1, 1, g).start()
        if g == 0:
            for s in range(OWN):
                lat_start(OWN + s)

    def zero_pads(n, carry):
        xs[n // SPAN, lax.rem(n, SPAN), ZROWS:256, :] = jnp.zeros((256 - ZROWS, LON), BF16)
        return carry

    lax.fori_loop(0, (ROWS + 2) * SPAN, zero_pads, 0)
    for rho in range(ROWS + 2):
        for t in range(OWN):
            rs[rho, t, ZROWS:256, :] = jnp.zeros((256 - ZROWS, LON), BF16)

    def zero_halo(rho):
        def one(e, carry):
            xs[rho, e, 0:ZROWS, :] = jnp.zeros((ZROWS, LON), BF16)
            return carry

        lax.fori_loop(0, SPAN, one, 0)
        for t in range(OWN):
            rs[rho, t, 0:ZROWS, :] = jnp.zeros((ZROWS, LON), BF16)
            gp[rho, t] = jnp.zeros((HID, LON), BF16)

    @pl.when(jnp.logical_not(has_up))
    def _():
        zero_halo(0)

    @pl.when(jnp.logical_not(has_down))
    def _():
        zero_halo(ROWS + 1)

    load_b1.wait()
    load_b2.wait()
    bi[...] = jnp.broadcast_to(b1[...][None, :], (HID, HID)).T
    row = jnp.concatenate([b2[...][None, :], jnp.zeros((1, 128 - C), F32)], axis=1)
    column = jnp.broadcast_to(row, (128, 128)).T
    bo[...] = jnp.concatenate([column[: MAIN + TAIL], column[: MAIN + TAIL]], axis=1)

    load_wi.wait()

    def weights(i, carry):
        for k in range(WINDOW):
            tails = []
            for j in range(3):
                low = (C * k) // 16 * 16
                high = min((C * k + C + 15) // 16 * 16, WINDOW * C)
                piece = wi[i, j, low:high, :].astype(F32)[C * k - low : C * k - low + C]
                main, tail = parts(piece)
                w4[i, k, 64 * j : 64 * j + 64, :] = main.astype(BF16)
                tails.append(tail)
            tails.append(jnp.zeros((MAIN - 3 * TAIL, HID), F32))
            w4[i, k, 192:256, :] = jnp.concatenate(tails, axis=0).astype(BF16)
            w1[i, k] = w4[i, k].T
        return carry

    lax.fori_loop(0, 3, weights, 0)
    load_wo.wait()
    for i in range(3):
        tails = []
        for j in range(3):
            main, tail = parts(wo[i, j].astype(F32))
            w2[i, 64 * j : 64 * j + 64, :] = main.astype(BF16)
            tails.append(tail)
        tails.append(jnp.zeros((MAIN - 3 * TAIL, HID), F32))
        w2[i, 192:256, :] = jnp.concatenate(tails, axis=0).astype(BF16)
        w2t[i] = w2[i].T

    def stack_chunk(e, g):
        chunk = chunk_of(e, g)
        tails = chunk[64:80, :].astype(F32)
        a, b = ((0, 3), (1, 2))[g]
        stack_into(xs.at[a + 1, e], chunk[0:64, :], tails[0:8], right, left)
        stack_into(xs.at[b + 1, e], chunk[80:144, :], tails[8:16], right, left)

    def stack_halo(e):
        @pl.when(has_up)
        def _():
            lat_copy(0, e, chunk_of(e, 0)).wait_recv()
            stack_into(xs.at[0, e], hb[0, e, 16:80, :], hb[0, e, 0:16, :].astype(F32)[8:16], right, left)

        @pl.when(has_down)
        def _():
            lat_copy(1, e, chunk_of(e, 0)).wait_recv()
            stack_into(xs.at[5, e], hb[1, e, 0:64, :], hb[1, e, 64:80, :].astype(F32)[0:8], right, left)

    for s in range(OWN):
        stack_chunk(OWN + s, 0)
        stack_chunk(OWN + s, 1)

    inner = ((0, 1), (1, 1), (0, 2), (1, 2))
    outer = ((0, 0), (1, 0), (0, 3), (1, 3))
    edge = {0: (1,), 1: (0,), 2: (2,), 3: (1,)}
    rest = {0: (2, 0), 1: (1, 2), 2: (0, 1), 3: (0, 2)}

    def conv_states(t, r, total, picks, taps=(0, 1, 2)):
        for e in picks:
            for i in taps:
                total = total + dot(w1[i, e - t], xs[r + i, e])
        return total

    def phase_own(t, r):
        pre[t, r] = conv_states(t, r, bi[...], (2, 3))

    def phase_near(t, r):
        pre[t, r] = conv_states(t, r, pre[t, r], (1, 4), rest[r])

    def phase_far(t, r):
        v = conv_states(t, r, pre[t, r], (5 * t,), rest[r])
        sig = 0.5 + 0.5 * jnp.tanh(0.5 * v)
        act[r, t] = (v * sig).astype(BF16)
        slope[r, t] = sig * (1.0 + v * (1.0 - sig))

    for t, r in inner:
        phase_own(t, r)
    for s in range(OWN):
        stack_halo(OWN + s)
    for t, r in outer:
        phase_own(t, r)

    tm_copy(0, 1, 0).wait_recv()
    lat_start(1)
    tm_copy(1, 0, 0).wait_recv()
    lat_start(4)
    stack_chunk(1, 0)
    stack_chunk(4, 0)
    tm_copy(0, 0, 0).wait_recv()
    lat_start(0)
    tm_copy(1, 1, 0).wait_recv()
    lat_start(5)
    stack_chunk(0, 0)
    stack_chunk(5, 0)
    for t, r in inner + outer:
        pre[t, r] = conv_states(t, r, pre[t, r], (1, 4, 5 * t), edge[r])
    tm_copy(0, 1, 1).wait_recv()
    tm_copy(1, 0, 1).wait_recv()
    stack_chunk(1, 1)
    stack_chunk(4, 1)
    for t, r in inner:
        phase_near(t, r)
    stack_halo(1)
    stack_halo(4)
    for t, r in outer:
        phase_near(t, r)
    load_ob.wait()
    stack_halo(0)
    stack_halo(5)
    tm_copy(0, 0, 1).wait_recv()
    tm_copy(1, 1, 1).wait_recv()
    stack_chunk(0, 1)
    stack_chunk(5, 1)
    for t in range(OWN):
        for r in (0, 1, 3, 2):
            phase_far(t, r)

    def score_terms(t, pairs):
        z = None
        for i, r in pairs:
            term = dot(w2[i, 0:ZROWS, :], act[r, t])
            z = term if z is None else z + term
        return combine(z, right, left)

    outer_terms = ((0, ((0, 3),), ((0, 2), (1, 3)), 3), (1, ((2, 0),), ((1, 0), (2, 1)), 0))
    for t in range(OWN):
        for d, given, kept, r in outer_terms:
            main, tail_c = score_terms(t, given)
            kc[d, t, 0:64, :] = main
            kc[d, t, 64:72, :] = tail_c
            sp[d, t, 0:64, :] = main.astype(BF16)
            main, tail = score_terms(t, kept)
            main = main + bo[0:64, :]
            tail = tail + bo[64:72, :]
            sc[r, t, 0:64, :] = main
            sc[r, t, 64:72, :] = tail
            seen_main, seen_tail = parts(row_of(ob, t, r))
            sp[d, t, 64:128, :] = (main - seen_main).astype(BF16)
            sp[d, t, 128:144, :] = jnp.concatenate([tail_c, tail - seen_tail], axis=0).astype(BF16)
        for d, present in ((0, has_down), (1, has_up)):
            @pl.when(present)
            def _():
                x2_copy(d, t).start()

    def finish_row(t, r, main, tail):
        seen_main, seen_tail = parts(row_of(ob, t, r))
        stack_into(rs.at[r + 1, t], (main - seen_main).astype(BF16), tail - seen_tail, left, right)

    for t in range(OWN):
        for r in (1, 2):
            main, tail = score_terms(t, tuple((i, r + i - 1) for i in range(3)))
            main = main + bo[0:64, :]
            tail = tail + bo[64:72, :]
            put_row(so, t, r, main, tail)
            finish_row(t, r, main, tail)

    for d, r, halo, present in ((0, 0, 0, has_up), (1, 3, 5, has_down)):
        @pl.when(present)
        def _():
            for t in range(OWN):
                x2_copy(d, t).wait_recv()
                tails = rp[d, t, 128:144, :].astype(F32)
                sc[r, t, 0:64, :] += rp[d, t, 0:64, :].astype(F32)
                sc[r, t, 64:72, :] += tails[0:8]
                main = kc[1 - d, t, 0:64, :] + rp[d, t, 64:128, :].astype(F32)
                tail = kc[1 - d, t, 64:72, :] + tails[8:16]
                stack_into(rs.at[halo, t], main.astype(BF16), tail, left, right)

    for t in range(OWN):
        for r in (0, 3):
            finish_row(t, r, sc[r, t, 0:64, :], sc[r, t, 64:72, :])

    def grad_hidden(t, r):
        total = None
        for i in range(3):
            term = dot(w2t[i], rs[r + 2 - i, t])
            total = term if total is None else total + term
        gp[r + 1, t] = (total * slope[r, t]).astype(BF16)

    def hidden_inner(n, carry):
        grad_hidden(lax.rem(n, OWN), 1 + n // OWN)
        return carry

    for t in range(OWN):
        for r in (3, 0):
            grad_hidden(t, r)
    for t in range(OWN):
        for d, present in ((0, has_down), (1, has_up)):
            @pl.when(present)
            def _():
                x3_copy(d, t).start()

    lax.fori_loop(0, 2 * OWN, hidden_inner, 0, unroll=True)

    def grad_state(e, r, taps=(0, 1, 2)):
        z = None
        for t in range(OWN):
            k = e - t
            if 0 <= k < WINDOW:
                for i in taps:
                    term = dot(w4[i, k, 0:ZROWS, :], gp[r + 2 - i, t])
                    z = term if z is None else z + term
        return combine(z, left, right)

    sides = ((1, 0), (0, 4))

    def pack_row(d, r, pair):
        (main_a, tail_a), (main_b, tail_b) = pair
        sg[d, r, 0:64, :] = main_a.astype(BF16)
        sg[d, r, 64:80, :] = jnp.concatenate([tail_a, tail_b], axis=0).astype(BF16)
        sg[d, r, 80:144, :] = main_b.astype(BF16)

    def own_rows(rows):
        for r in rows:
            for s in range(OWN):
                main, tail = grad_state(OWN + s, r)
                own[r, s, 0:64, :] = main
                own[r, s, 64:72, :] = tail

    for r in (1, 2):
        for d, e in sides:
            pack_row(d, r, [grad_state(e + s, r) for s in range(OWN)])
        for d, e in sides:
            g_copy(d, r).start()

    for t in range(OWN):
        for r in (0, 3):
            put_row(so, t, r, sc[r, t, 0:64, :], sc[r, t, 64:72, :])

    for n, (r, taps) in enumerate(((0, (0, 1)), (3, (1, 2)))):
        for d, e in sides:
            for s in range(OWN):
                main, tail = grad_state(e + s, r, taps)
                near[n, d, s, 0:64, :] = main
                near[n, d, s, 64:72, :] = tail
    own_rows((1, 2))

    for n, (r, tap, present) in enumerate(((0, 2, has_up), (3, 0, has_down))):
        @pl.when(present)
        def _():
            for t in range(OWN):
                x3_copy(n, t).wait_recv()

        for d, e in sides:
            pair = []
            for s in range(OWN):
                main, tail = grad_state(e + s, r, (tap,))
                pair.append((main + near[n, d, s, 0:64, :], tail + near[n, d, s, 64:72, :]))
            pack_row(d, r, pair)
        for d, e in sides:
            g_copy(d, r).start()

    own_rows((0, 3))

    for d in range(2):
        remote(sbuf, rbuf.at[d], tm_send.at[d], tm_recv.at[d, 0, 0], (nxt, l)).wait_send()

        @pl.when(has_down if d == 0 else has_up)
        def _():
            remote(hb.at[d], hb.at[d], lat_send.at[d], lat_recv.at[d, 0], (nxt, l)).wait_send()
            for t in range(OWN):
                x2_copy(d, t).wait_send()
                x3_copy(d, t).wait_send()

    for r in (1, 2, 0, 3):
        g_copy(0, r).wait_recv()
        g_copy(1, r).wait_recv()
        tails = rg[0, r, 64:80, :].astype(F32) + rg[1, r, 64:80, :].astype(F32)
        for s in range(OWN):
            low = 80 * s
            main = own[r, s, 0:64, :] + rg[0, r, low : low + 64, :].astype(F32) + rg[1, r, low : low + 64, :].astype(F32)
            tail = own[r, s, 64:72, :] + tails[8 * s : 8 * s + 8]
            put_row(go, s, r, main, tail)

    for d in range(2):
        remote(sg.at[d], rg.at[d], g_send.at[d], g_recv.at[d, 0], (nxt, l)).wait_send()


def write_out(so, go, scores_out, guidance_out, sems):
    copies = []
    for s in range(OWN):
        copies.append(pltpu.make_async_copy(so.at[s], scores_out.at[s], sems.at[0, s]))
        copies.append(pltpu.make_async_copy(go.at[s], guidance_out.at[s], sems.at[1, s]))
    for copy in copies:
        copy.start()
    for copy in copies:
        copy.wait()


def solution(mesh):
    whole = P("tm", None, "lat", None)

    def step(states, observed, conv_in, bias_in, conv_out, bias_out):
        shape = states.shape
        dma = pltpu.SemaphoreType.DMA
        hbm = pl.BlockSpec(memory_space=pltpu.HBM)
        vmem = pl.BlockSpec(memory_space=pltpu.VMEM)
        view = (shape[0], shape[1] * shape[2] * 2, 128)

        def seen(x):
            halves = x.reshape(shape[0], shape[1], shape[2], 2, 128)
            return jnp.transpose(halves, (0, 1, 3, 2, 4)).reshape(view)

        def unseen(x):
            halves = x.reshape(shape[0], shape[1], 2, shape[2], 128)
            return jnp.transpose(halves, (0, 1, 3, 2, 4)).reshape(shape)

        so, go = pl.pallas_call(
            kernel,
            out_shape=(pltpu.VMEM(view, F32), pltpu.VMEM(view, F32)),
            in_specs=[hbm] * 6,
            out_specs=(vmem, vmem),
            scratch_shapes=[
                pltpu.VMEM(view, F32),
                pltpu.VMEM(view, F32),
                pltpu.VMEM((3, 3, WINDOW * C, HID), BF16),
                pltpu.VMEM((3, 3, C, HID), BF16),
                pltpu.VMEM((3, WINDOW, 256, HID), BF16),
                pltpu.VMEM((3, WINDOW, HID, 256), BF16),
                pltpu.VMEM((3, 256, HID), BF16),
                pltpu.VMEM((3, HID, 256), BF16),
                pltpu.VMEM((HID, LON), F32),
                pltpu.VMEM((MAIN + TAIL, LON), F32),
                pltpu.VMEM((OWN, 2, CHUNK, LON), BF16),
                pltpu.VMEM((2, OWN, 2, CHUNK, LON), BF16),
                pltpu.VMEM((2, SPAN, EDGE, LON), BF16),
                pltpu.VMEM((ROWS + 2, SPAN, 256, LON), BF16),
                pltpu.VMEM((OWN, ROWS, HID, LON), F32),
                pltpu.VMEM((ROWS, OWN, HID, LON), F32),
                pltpu.VMEM((ROWS, OWN, HID, LON), BF16),
                pltpu.VMEM((2, OWN, CHUNK, LON), BF16),
                pltpu.VMEM((2, OWN, CHUNK, LON), BF16),
                pltpu.VMEM((2, OWN, MAIN + TAIL, LON), F32),
                pltpu.VMEM((ROWS, OWN, MAIN + TAIL, LON), F32),
                pltpu.VMEM((ROWS + 2, OWN, 256, LON), BF16),
                pltpu.VMEM((ROWS + 2, OWN, HID, LON), BF16),
                pltpu.VMEM((2, ROWS, CHUNK, LON), BF16),
                pltpu.VMEM((2, ROWS, CHUNK, LON), BF16),
                pltpu.VMEM((ROWS, OWN, MAIN + TAIL, LON), F32),
                pltpu.VMEM((2, 2, OWN, MAIN + TAIL, LON), F32),
                pltpu.VMEM((HID,), F32),
                pltpu.VMEM((C,), F32),
                dma((6,)),
                dma((2,)),
                dma((2, OWN, 2)),
                dma((2,)),
                dma((2, SPAN)),
                dma((2, OWN)),
                dma((2, OWN)),
                dma((2, OWN)),
                dma((2, OWN)),
                dma((2,)),
                dma((2, ROWS)),
            ],
            compiler_params=pltpu.CompilerParams(
                collective_id=0, has_side_effects=True, vmem_limit_bytes=60 * 1024 * 1024
            ),
        )(seen(states), seen(observed), jnp.transpose(conv_in, (0, 1, 3, 2)), bias_in, conv_out, bias_out)
        so, go = (pltpu.with_memory_space_constraint(x, pltpu.VMEM) for x in (so, go))
        scores, guidance = pl.pallas_call(
            write_out,
            out_shape=(jax.ShapeDtypeStruct(view, F32), jax.ShapeDtypeStruct(view, F32)),
            in_specs=[vmem, vmem],
            out_specs=(hbm, hbm),
            scratch_shapes=[dma((2, OWN))],
            compiler_params=pltpu.CompilerParams(vmem_limit_bytes=4 * 1024 * 1024),
        )(so, go)
        return unseen(scores), unseen(guidance)

    sharded = jax.shard_map(
        step, mesh=mesh, in_specs=(whole, whole, P(), P(), P(), P()), out_specs=(whole, whole), check_vma=False
    )

    def run(*args):
        with jax.sharding.use_abstract_mesh(mesh.abstract_mesh):
            return sharded(*args)

    return run
```
